32 devices in a mesh: dp: 4 (over z), seq: 8 (over y, x, core).
Axes of the slice: x: 2, y: 2, z: 4, core: 2. Of those that a mesh axis runs over, the one named last changes fastest.
Arguments:
- queries: bfloat16 [4096, 64, 128], P(('dp', 'seq')), parts along dimension 0, may hold values from -52 to 52
- keys: bfloat16 [4096, 8, 128], P(('dp', 'seq')), parts along dimension 0, may hold values from -6 to 6
- values: bfloat16 [4096, 8, 128], P(('dp', 'seq')), parts along dimension 0, may hold values from -6 to 6
- doc_ids: int32 [4096], P(('dp', 'seq')), parts along dimension 0, may hold values from 0 to 7, never falling along the last dimension, each value on 1 to 512 neighbouring positions
- counts: int32 [32], P('dp'), parts along dimension 0, may hold values from 64 to 128
Outputs:
- attended: bfloat16 [4096, 64, 128], P(('dp', 'seq')), parts along dimension 0
The draws below stay inside these ranges and needn't reach their ends.
There are 4 independent parts, one for each index of `dp`. The reference program is written for one: setup_inputs(seed, part) draws one part's arguments, and reference() takes and returns one part's arrays. A program takes and returns all parts, laid end to end along the dimension named above; each array names one. Nothing has to cross between parts.
Inputs may be any that keep to these rules, and one draw needn't show every extreme that they name: `doc_ids`: document numbers never fall along the sequence; each document has 1 to 512 positions. The first counts[j] positions of shard j are real tokens, the others padding.
All inputs are finite; a program needn't handle non-finite values.
Results may differ from the reference program's by a relative error of at most 0.003.
Values may be sent and summed in bfloat16 or wider, within the bound.
A program may use at most 64 MiB of HBM per device.

```python
import math
import jax
import jax.numpy as jnp
import numpy as np
from jax import lax

QUERY_HEAD_COUNT = 64
KEY_VALUE_HEADS = 8
HEAD_WIDTH = 128
S_DEV = 128
BLOCK_POSITIONS = 512
DOC_MOST = 512
SEQUENCE_LENGTH = 1024
DOCS = 8
N_SEQ = 8


def draw_pair(key):
    base = jax.random.fold_in(key, 11)
    key_query, key_random_seed = jax.random.split(base)
    query_draw = jnp.clip(jax.random.normal(key_query, (SEQUENCE_LENGTH, QUERY_HEAD_COUNT, HEAD_WIDTH), jnp.float32), -6.0, 6.0)
    key_sample = jnp.clip(jax.random.normal(key_random_seed, (SEQUENCE_LENGTH, KEY_VALUE_HEADS, HEAD_WIDTH), jnp.float32), -6.0, 6.0)
    return (query_draw, key_sample)


def draw_queries(key, part):
    return draw_pair(key)[0].astype(jnp.bfloat16)


def draw_keys(key, part):
    return draw_pair(key)[1].astype(jnp.bfloat16)


def plant(values, stream_key, low, largest):
    longest = values.shape.index(max(values.shape))
    spots = []
    for shift in (0, 1):
        where = [jax.random.randint(jax.random.fold_in(stream_key, axis), (), 0, length) for axis, length in enumerate(values.shape)]
        where[longest] = (where[longest] + shift) % values.shape[longest]
        spots.append(tuple(where))
    return values.at[spots[0]].set(low).at[spots[1]].set(largest)


def levels(rng, extent, cuts, least, top_value):
    loudness = 1.0
    for dim, blocks in cuts:
        draws = jax.random.uniform(jax.random.fold_in(jax.random.fold_in(rng, 6), dim), (blocks,), jnp.float32, least / len(cuts), top_value / len(cuts))
        loudness = loudness * jnp.repeat(jnp.exp(draws), extent[dim] // blocks).reshape((-1,) + (1,) * (len(extent) - 1 - dim))
    return loudness


def profile(amount, total, most, skew):
    portions = [(1 << 20) // math.isqrt(rank ** skew) + 1 for rank in range(2, amount + 1)]
    surplus, holding = total - most - (amount - 1), [1] * (amount - 1)
    while surplus > 0:
        movable = [i for i in range(amount - 1) if holding[i] < most]
        whole, left = sum([portions[i] for i in movable]), surplus
        for i in movable:
            extra = min(most - holding[i], max(1, left * portions[i] // whole), surplus)
            holding[i] = holding[i] + extra
            surplus = surplus - extra
    return np.array([most] + holding)


def ragged(rng, count, total, most, lean):
    if count == 2:
        one = jax.random.randint(rng, (), max(1, total - most), min(most, total - 1) + 1)
        return jnp.stack([one, total - one])
    lengths = jnp.asarray(profile(count, total, most, lean), jnp.int32)
    twos = (count - 1) // 2
    donor, taker = lengths[1:1 + 2 * twos:2], lengths[2:2 + 2 * twos:2]
    margin = jnp.minimum(donor - 1, most - taker)
    shifted = jax.random.randint(jax.random.fold_in(rng, 1), (twos,), 0, 1 << 20) % (margin + 1)
    lengths = lengths.at[1:1 + 2 * twos:2].set(donor - shifted).at[2:2 + 2 * twos:2].set(taker + shifted)
    return lengths[jax.random.permutation(jax.random.fold_in(rng, 2), count)]


def centred(key, shape, spread, reach, shards=(), held_as=jnp.bfloat16):
    values = spread * jax.random.normal(key, shape, jnp.float32)
    if shards:
        values = values * levels(key, shape, shards, -0.22, 0.18)
    return jnp.clip(values, -reach, reach).astype(held_as)


def setup_inputs(seed: int = 0, part: int = 0) -> dict:
    seeds = jax.random.split(jax.random.key(seed), 6)
    part_keys = jax.random.split(jax.random.fold_in(seeds[5], part), 6)
    return {
        "queries": draw_queries(jax.random.fold_in(jax.random.fold_in(seeds[5], part), 71), part),
        "keys": draw_keys(jax.random.fold_in(jax.random.fold_in(seeds[5], part), 71), part),
        "values": centred(part_keys[2], (SEQUENCE_LENGTH, KEY_VALUE_HEADS, HEAD_WIDTH), 1.0, 6.0, ((0, 8),)),
        "doc_ids": jnp.searchsorted(jnp.cumsum(ragged(part_keys[3], DOCS, SEQUENCE_LENGTH, DOC_MOST, 2)), jnp.arange(SEQUENCE_LENGTH), side="right").astype(jnp.int32),
        "counts": plant(jax.random.randint(part_keys[4], (N_SEQ,), S_DEV // 2, S_DEV + 1), jax.random.fold_in(part_keys[4], 1), S_DEV // 2, S_DEV).astype(jnp.int32),
    }


def reference(queries, keys, values, doc_ids, counts):
    row_count = queries.shape[0]
    shard_rows = row_count // N_SEQ
    queries_per_group = QUERY_HEAD_COUNT // KEY_VALUE_HEADS
    score_scale = 1.0 / math.sqrt(HEAD_WIDTH)
    positions = jnp.arange(row_count, dtype=jnp.int32)
    live_rows = positions % shard_rows < jnp.repeat(counts, shard_rows, total_repeat_length=row_count)
    keys_float = keys.astype(jnp.float32)
    values_float = values.astype(jnp.float32)

    def one_block(start):
        query_tile_rows = lax.dynamic_slice_in_dim(queries, start, BLOCK_POSITIONS, 0).astype(jnp.float32)
        query_tile_rows = query_tile_rows.reshape(BLOCK_POSITIONS, KEY_VALUE_HEADS, queries_per_group, HEAD_WIDTH)
        scores = jnp.einsum('qhgd,khd->hgqk', query_tile_rows, keys_float, precision=lax.Precision.HIGHEST) * score_scale
        query_pos = start + jnp.arange(BLOCK_POSITIONS, dtype=jnp.int32)
        query_doc = lax.dynamic_slice_in_dim(doc_ids, start, BLOCK_POSITIONS, 0)
        query_live = lax.dynamic_slice_in_dim(live_rows, start, BLOCK_POSITIONS, 0)
        allowed = (doc_ids[None, :] == query_doc[:, None]) & (positions[None, :] <= query_pos[:, None]) & live_rows[None, :]
        masked = jnp.where(allowed, scores, -1e+30)
        top = lax.optimization_barrier(jnp.max(masked, axis=-1, keepdims=True))
        weights = jnp.where(allowed, jnp.exp(scores - top), 0.0)
        norm_sum = lax.optimization_barrier(jnp.sum(weights, axis=-1))
        rounded = weights.astype(jnp.bfloat16).astype(jnp.float32)
        mixed = jnp.einsum('hgqk,khd->qhgd', rounded, values_float, precision=lax.Precision.HIGHEST)
        norm_rows = jnp.transpose(norm_sum, (2, 0, 1))[:, :, :, None]
        norm_rows = jnp.where(query_live[:, None, None, None], norm_rows, 1.0)
        output = jnp.where(query_live[:, None, None, None], mixed / norm_rows, 0.0)
        return output.reshape(BLOCK_POSITIONS, QUERY_HEAD_COUNT, HEAD_WIDTH).astype(jnp.bfloat16)
    starts = jnp.arange(0, row_count, BLOCK_POSITIONS, dtype=jnp.int32)
    blocks = lax.map(one_block, starts)
    return blocks.reshape(row_count, QUERY_HEAD_COUNT, HEAD_WIDTH)
```

```python
import functools
import math

import jax
import jax.numpy as jnp
from jax import lax
from jax.experimental import pallas as pl
from jax.experimental.pallas import tpu as pltpu
from jax.sharding import PartitionSpec as P

DOC_MOST = 512
MESH = pl.DeviceIdType.MESH
NEG = -1e30


def kernel(
    n, reach, tile,
    counts_hbm, q_hbm, k_hbm, v_hbm, docs_hbm, out_ref,
    raw, win, q_vmem, dwin, bias, counts_ref, small_sem, raw_sem,
    q_sem, send_sem, recv_sem, dsend_sem, drecv_sem,
):
    me = lax.axis_index("seq")
    heads, shard_rows, group, width = q_vmem.shape
    blocks = reach + 1
    keys_all = blocks * shard_rows
    rows = shard_rows * group
    tree = n == 8 and reach == 4

    even = lax.rem(me, 2) == 0
    odd = jnp.logical_not(even)
    chip_odd = lax.rem(me // 2, 2) == 1
    partner = me + 1 - 2 * lax.rem(me, 2)
    if tree:
        own_sends = [
            (0, jnp.logical_not(chip_odd), 2),
            (1, me < 4, 4),
            (2, even, 1),
        ]
        senders = [
            (odd | (me >= 2), partner),
            (chip_odd, me - 2),
            (me >= 4, me - 4),
            ((me >= 4) & (me < 6), me + 2),
        ]
        targets = [even | (me >= 2), jnp.logical_not(chip_odd), me < 4, me >= 6]
    else:
        own_sends = [(off - 1, me + off < n, off) for off in range(1, reach + 1)]
        senders = [(me >= off, me - off) for off in range(1, reach + 1)]
        targets = [me + off < n for off in range(1, reach + 1)]

    barrier = pltpu.get_barrier_semaphore()
    for cond, device in senders:
        @pl.when(cond)
        def _(device=device):
            pl.semaphore_signal(
                barrier, inc=1, device_id={"seq": lax.rem(device + n, n)},
                device_id_type=MESH,
            )

    def loop(body, count=None):
        lax.fori_loop(0, heads if count is None else count, lambda i, c: (body(i), c)[1], 0)

    raw_copies = [
        pltpu.make_async_copy(ref, raw.at[part], raw_sem.at[part])
        for part, ref in enumerate((k_hbm, v_hbm))
    ]
    doc_copy = pltpu.make_async_copy(docs_hbm, dwin.at[reach], small_sem.at[0])
    count_copy = pltpu.make_async_copy(counts_hbm, counts_ref, small_sem.at[1])
    doc_copy.start()
    for copy in raw_copies:
        copy.start()
    count_copy.start()

    def q_copy(h):
        return pltpu.make_async_copy(q_hbm.at[:, h], q_vmem.at[h], q_sem.at[h])

    def send(item, kind, from_off, to, to_off):
        if item is None:
            src, dst = dwin.at[reach - from_off], dwin.at[reach - to_off]
            sems = dsend_sem.at[kind], drecv_sem.at[to_off - 1]
        else:
            h, part = item
            src, dst = win.at[h, part, reach - from_off], win.at[h, part, reach - to_off]
            sems = send_sem.at[h, part, kind], recv_sem.at[h, part, to_off - 1]
        return pltpu.make_async_remote_copy(
            src_ref=src, dst_ref=dst, send_sem=sems[0], recv_sem=sems[1],
            device_id={"seq": to}, device_id_type=MESH,
        )

    def wait_block(item, off):
        send(item, 0, 0, lax.rem(me + 1, n), off).wait_recv()

    def start_own(item):
        for kind, cond, off in own_sends:
            @pl.when(cond)
            def _(kind=kind, off=off):
                send(item, kind, 0, lax.rem(me + off, n), off).start()

    doc_copy.wait()
    for part in range(2):
        raw_copies[part].wait()
        win[:, part, reach] = jnp.swapaxes(raw[part], 0, 1)
    pl.semaphore_wait(barrier, sum(jnp.where(cond, 1, 0) for cond in targets))

    start_own(None)

    def start_head(h):
        for part in range(2):
            start_own((h, part))

    loop(start_head)
    loop(lambda h: q_copy(h).start())
    count_copy.wait()

    for off in range(1, reach + 1):
        @pl.when(me < off)
        def _(off=off):
            dwin[reach - off] = jnp.full(dwin.shape[1:], -1, jnp.int32)

            def clear(h):
                win[h, :, reach - off] = jnp.zeros((2, shard_rows, width), win.dtype)

            loop(clear)

    def relay_two(item):
        wait_block(item, 2)

        @pl.when(even)
        def _():
            send(item, 3, 2, partner, 3).start()

        @pl.when(odd)
        def _():
            send(item, 3, 2, partner, 1).start()

    def relay_four(item):
        wait_block(item, 4)

        @pl.when(me >= 6)
        def _():
            send(item, 5, 4, me - 2, 2).start()

        @pl.when(odd)
        def _():
            send(item, 4, 4, me - 1, 3).start()

    def relay(item):
        @pl.when(me >= 4)
        def _():
            relay_four(item)

        @pl.when(me >= 2)
        def _():
            relay_two(item)

    def arrivals(item, offs):
        for off in offs:
            @pl.when(me >= off)
            def _(off=off):
                wait_block(item, off)

    if tree:
        relay(None)
        arrivals(None, (1, 3))
    else:
        arrivals(None, range(1, reach + 1))

    lane = lax.broadcasted_iota(jnp.int32, (shard_rows, shard_rows), 1)
    row = lax.broadcasted_iota(jnp.int32, (shard_rows, shard_rows), 0)
    doc_col = jnp.transpose(jnp.broadcast_to(dwin[reach], (shard_rows, shard_rows)))
    for slot in range(blocks):
        off = reach - slot
        count = counts_ref[lax.max(me - off, 0)]
        docs = dwin[slot]
        allowed = (docs == doc_col) & (lane < count)
        if off == 0:
            allowed = allowed & (lane <= row)
        part = jnp.where(allowed, 0.0, NEG).astype(jnp.float32)
        part = jnp.broadcast_to(part[:, None, :], (shard_rows, group, shard_rows))
        bias[:, slot * shard_rows : (slot + 1) * shard_rows] = part.reshape(rows, shard_rows)

    own_count = counts_ref[me]
    factor = math.log2(math.e) / math.sqrt(width)

    def attend(h):
        q_copy(h).wait()
        keys = win[h, 0].reshape(keys_all, width)
        values = win[h, 1].reshape(keys_all, width)

        def scores(start):
            q = q_vmem[h, start // group : (start + tile) // group].reshape(tile, width)
            return lax.dot_general(
                q, keys, (((1,), (1,)), ((), ())), preferred_element_type=jnp.float32
            )

        s_next = scores(0)
        for start in range(0, rows, tile):
            s = s_next
            if start + tile < rows:
                s_next = scores(start + tile)
            x = s * factor + bias[start : start + tile, :]
            top = jnp.max(x, axis=-1, keepdims=True)
            p = jnp.exp2(x - top)
            norm = jnp.sum(p, axis=-1, keepdims=True)
            o = lax.dot_general(
                p.astype(jnp.bfloat16), values, (((1,), (0,)), ((), ())),
                preferred_element_type=jnp.float32,
            )
            r = lax.broadcasted_iota(jnp.int32, (tile, width), 0) + start
            o = jnp.where(r < own_count * group, o / norm, 0.0).astype(jnp.bfloat16)
            out_ref[start // group : (start + tile) // group, h] = o.reshape(
                tile // group, group, width
            )

    def step(it):
        if tree:
            @pl.when(it < heads)
            def _():
                for part in range(2):
                    relay((it, part))

            @pl.when(it >= 1)
            def _():
                for part in range(2):
                    arrivals((it - 1, part), (1, 3))
                attend(it - 1)
        else:
            for part in range(2):
                arrivals((it, part), range(1, reach + 1))
            attend(it)

    loop(step, heads + 1 if tree else heads)

    def finish(item):
        for kind, cond, off in own_sends:
            @pl.when(cond)
            def _(kind=kind, off=off):
                send(item, kind, 0, lax.rem(me + off, n), off).wait_send()
        if tree:
            @pl.when(me >= 2)
            def _():
                send(item, 3, 2, partner, 1).wait_send()

            @pl.when((me >= 4) & odd)
            def _():
                send(item, 4, 4, me - 1, 3).wait_send()

            @pl.when(me >= 6)
            def _():
                send(item, 5, 4, me - 2, 2).wait_send()

    finish(None)

    def finish_head(h):
        for part in range(2):
            finish((h, part))

    loop(finish_head)


def local(n, queries, keys, values, doc_ids, counts):
    shard_rows, q_heads, width = queries.shape
    heads = keys.shape[1]
    group = q_heads // heads
    reach = min((DOC_MOST + shard_rows - 1) // shard_rows, n - 1)
    rows = shard_rows * group
    out = pl.pallas_call(
        functools.partial(kernel, n, reach, 512),
        out_shape=pltpu.VMEM((shard_rows, heads, group, width), jnp.bfloat16),
        in_specs=[pl.BlockSpec(memory_space=pltpu.HBM)] * 5,
        out_specs=pl.BlockSpec(memory_space=pltpu.VMEM),
        scratch_shapes=[
            pltpu.VMEM((2, shard_rows, heads, width), jnp.bfloat16),
            pltpu.VMEM((heads, 2, reach + 1, shard_rows, width), jnp.bfloat16),
            pltpu.VMEM((heads, shard_rows, group, width), jnp.bfloat16),
            pltpu.VMEM((reach + 1, 1, shard_rows), jnp.int32),
            pltpu.VMEM((rows, (reach + 1) * shard_rows), jnp.float32),
            pltpu.SMEM(counts.shape, jnp.int32),
            pltpu.SemaphoreType.DMA((2,)),
            pltpu.SemaphoreType.DMA((2,)),
            pltpu.SemaphoreType.DMA((heads,)),
            pltpu.SemaphoreType.DMA((heads, 2, 6)),
            pltpu.SemaphoreType.DMA((heads, 2, reach)),
            pltpu.SemaphoreType.DMA((6,)),
            pltpu.SemaphoreType.DMA((reach,)),
        ],
        compiler_params=pltpu.CompilerParams(
            collective_id=0, has_side_effects=True, vmem_limit_bytes=51 << 20
        ),
    )(
        *(
            pltpu.with_memory_space_constraint(x, pltpu.HBM)
            for x in (
                counts,
                queries.reshape(shard_rows, heads, group, width),
                keys,
                values,
                doc_ids.reshape(1, shard_rows),
            )
        )
    )
    return out.reshape(shard_rows, q_heads, width)


def solution(mesh):
    in_specs = (
        P(("dp", "seq"), None, None),
        P(("dp", "seq"), None, None),
        P(("dp", "seq"), None, None),
        P(("dp", "seq")),
        P("dp"),
    )
    out_specs = P(("dp", "seq"), None, None)
    return jax.shard_map(
        functools.partial(local, mesh.shape["seq"]),
        mesh=mesh, in_specs=in_specs, out_specs=out_specs, check_vma=False,
    )
```

```python
import functools
import math

import jax
import jax.numpy as jnp
from jax import lax
from jax.experimental import pallas as pl
from jax.experimental.pallas import tpu as pltpu
from jax.sharding import PartitionSpec as P

DOC_MOST = 512
MESH = pl.DeviceIdType.MESH
NEG = -1e30


def kernel(
    n, reach, tile,
    counts_hbm, q_hbm, k_hbm, v_hbm, docs_hbm, out_ref,
    raw, win, q_vmem, dwin, bias, top_ref, norm_ref, part_ref, counts_ref, small_sem, raw_sem,
    q_sem, send_sem, recv_sem, dsend_sem, drecv_sem,
):
    me = lax.axis_index("seq")
    heads, shard_rows, group, width = q_vmem.shape
    blocks = reach + 1
    rows = shard_rows * group
    tree = n == 8 and reach == 4

    even = lax.rem(me, 2) == 0
    odd = jnp.logical_not(even)
    chip_odd = lax.rem(me // 2, 2) == 1
    partner = me + 1 - 2 * lax.rem(me, 2)
    if tree:
        own_sends = [
            (0, jnp.logical_not(chip_odd), 2),
            (1, me < 4, 4),
            (2, even, 1),
        ]
        senders = [
            (odd | (me >= 2), partner),
            (chip_odd | (me == 4) | (me == 5), me - 2),
            (me >= 4, me - 4),
            ((me >= 4) & (me < 6), me + 2),
        ]
        targets = [even | (me >= 2), (me < 4) | jnp.logical_not(chip_odd), me < 4, me >= 6]
        straight = (me == 2) | (me == 3)
        send_shift = jnp.where(me >= 2, 1, 0)
        shift = jnp.where(me >= 6, 1, 0)
    else:
        own_sends = [(off - 1, me + off < n, off) for off in range(1, reach + 1)]
        senders = [(me >= off, me - off) for off in range(1, reach + 1)]
        targets = [me + off < n for off in range(1, reach + 1)]
        send_shift = shift = 0

    barrier = pltpu.get_barrier_semaphore()
    for cond, device in senders:
        @pl.when(cond)
        def _(device=device):
            pl.semaphore_signal(
                barrier, inc=1, device_id={"seq": lax.rem(device + n, n)},
                device_id_type=MESH,
            )

    def loop(body, count=None):
        lax.fori_loop(0, heads if count is None else count, lambda i, c: (body(i), c)[1], 0)

    raw_copies = [
        pltpu.make_async_copy(ref, raw.at[part], raw_sem.at[part])
        for part, ref in enumerate((k_hbm, v_hbm))
    ]
    doc_copy = pltpu.make_async_copy(docs_hbm, dwin.at[reach], small_sem.at[0])
    count_copy = pltpu.make_async_copy(counts_hbm, counts_ref, small_sem.at[1])
    doc_copy.start()
    for copy in raw_copies:
        copy.start()
    count_copy.start()

    def q_copy(h):
        return pltpu.make_async_copy(q_hbm.at[:, h], q_vmem.at[h], q_sem.at[h])

    loop(lambda h: q_copy(h).start())

    def send(item, kind, from_off, to, to_off):
        if item is None:
            src, dst = dwin.at[reach - from_off], dwin.at[reach - to_off]
            sems = dsend_sem.at[kind], drecv_sem.at[to_off - 1]
        else:
            h, part = item
            src, dst = win.at[h, part, reach - from_off], win.at[h, part, reach - to_off]
            sems = send_sem.at[h, part, kind], recv_sem.at[h, part, to_off - 1]
        return pltpu.make_async_remote_copy(
            src_ref=src, dst_ref=dst, send_sem=sems[0], recv_sem=sems[1],
            device_id={"seq": to}, device_id_type=MESH,
        )

    def wait_block(item, off):
        send(item, 0, 0, lax.rem(me + 1, n), off).wait_recv()

    def start_own(item):
        for kind, cond, off in own_sends:
            @pl.when(cond)
            def _(kind=kind, off=off):
                send(item, kind, 0, lax.rem(me + off, n), off).start()

    doc_copy.wait()
    for part in range(2):
        raw_copies[part].wait()
        win[:, part, reach] = jnp.swapaxes(raw[part], 0, 1)
    pl.semaphore_wait(barrier, sum(jnp.where(cond, 1, 0) for cond in targets))

    start_own(None)
    if tree:
        @pl.when(straight)
        def _():
            for item in (None, (0, 0), (0, 1)):
                send(item, 6, 0, me + 2, 2).start()

    def start_head(i):
        for part in range(2):
            start_own((lax.rem(i + send_shift, heads), part))

    loop(start_head)
    count_copy.wait()

    for off in range(1, reach + 1):
        @pl.when(me < off)
        def _(off=off):
            dwin[reach - off] = jnp.full(dwin.shape[1:], -1, jnp.int32)

            def clear(h):
                win[h, :, reach - off] = jnp.zeros((2, shard_rows, width), win.dtype)

            loop(clear)

    def relay_two(item):
        wait_block(item, 2)

        @pl.when(even)
        def _():
            send(item, 3, 2, partner, 3).start()

        @pl.when(odd)
        def _():
            send(item, 3, 2, partner, 1).start()

    def relay_four(item):
        wait_block(item, 4)

        if item is not None:
            @pl.when((me >= 6) & (item[0] > 0))
            def _():
                send(item, 5, 4, me - 2, 2).start()

        @pl.when(odd)
        def _():
            send(item, 4, 4, me - 1, 3).start()

    def relay(item):
        @pl.when(me >= 4)
        def _():
            relay_four(item)

        @pl.when(me >= 2)
        def _():
            relay_two(item)

    def arrivals(item, offs):
        for off in offs:
            @pl.when(me >= off)
            def _(off=off):
                wait_block(item, off)

    lane = lax.broadcasted_iota(jnp.int32, (shard_rows, shard_rows), 1)
    row = lax.broadcasted_iota(jnp.int32, (shard_rows, shard_rows), 0)
    doc_col = jnp.transpose(jnp.broadcast_to(dwin[reach], (shard_rows, shard_rows)))

    def fill_bias(slot):
        off = reach - slot
        count = counts_ref[lax.max(me - off, 0)]
        docs = dwin[slot]
        allowed = (docs == doc_col) & (lane < count)
        if off == 0:
            allowed = allowed & (lane <= row)
        part = jnp.where(allowed, 0.0, NEG).astype(jnp.float32)
        part = jnp.broadcast_to(part[:, None, :], (shard_rows, group, shard_rows))
        bias[:, slot * shard_rows : (slot + 1) * shard_rows] = part.reshape(rows, shard_rows)

    own_count = counts_ref[me]
    factor = math.log2(math.e) / math.sqrt(width)
    remote = reach * shard_rows
    together = math.gcd(heads, 4)

    def scores(h, start, keys):
        q = q_vmem[h, start // group : (start + tile) // group].reshape(tile, width)
        return lax.dot_general(
            q, keys, (((1,), (1,)), ((), ())), preferred_element_type=jnp.float32
        )

    def mix(p, values):
        return lax.dot_general(
            p.astype(jnp.bfloat16), values, (((1,), (0,)), ((), ())),
            preferred_element_type=jnp.float32,
        )

    def own_scores(h):
        q_copy(h).wait()
        q = q_vmem[h].reshape(rows, width)
        return lax.dot_general(
            q, win[h, 0, reach], (((1,), (1,)), ((), ())), preferred_element_type=jnp.float32
        )

    def own_weights(h, s):
        x = s * factor + bias[:, remote:]
        top = jnp.max(x, axis=-1, keepdims=True)
        top_ref[h] = jnp.broadcast_to(top, (rows, width))
        return jnp.exp2(x - top)

    def own_mix(h, p):
        ones = jnp.ones((shard_rows, width), jnp.bfloat16)
        o = mix(p, jnp.concatenate([win[h, 1, reach], ones], axis=1))
        part_ref[h] = o[:, :width]
        norm_ref[h] = o[:, width:]

    def attend_own(i):
        hs = [i * together + u for u in range(together)]
        s, p = {}, {}
        for k in range(together + 2):
            if k < together:
                s[k] = own_scores(hs[k])
            if 1 <= k <= together:
                p[k - 1] = own_weights(hs[k - 1], s.pop(k - 1))
            if k >= 2:
                own_mix(hs[k - 2], p.pop(k - 2))

    def attend(h):
        keys = win[h, 0, :reach].reshape(remote, width)
        values = win[h, 1, :reach].reshape(remote, width)
        s_next = scores(h, 0, keys)
        for start in range(0, rows, tile):
            at = slice(start, start + tile)
            s = s_next
            if start + tile < rows:
                s_next = scores(h, start + tile, keys)
            x = s * factor + bias[at, :remote]
            own_top = top_ref[h, at]
            top = jnp.maximum(jnp.max(x, axis=-1, keepdims=True), own_top)
            p = jnp.exp2(x - jnp.concatenate([top] * reach, axis=1))
            own = jnp.exp2(own_top - top)
            norm = jnp.sum(p, axis=-1, keepdims=True) + own * norm_ref[h, at]
            o = mix(p, values) + own * part_ref[h, at]
            r = lax.broadcasted_iota(jnp.int32, (tile, width), 0) + start
            o = jnp.where(r < own_count * group, o / norm, 0.0).astype(jnp.bfloat16)
            out_ref[start // group : (start + tile) // group, h] = o.reshape(
                tile // group, group, width
            )

    def order(i):
        return lax.rem(i + shift, heads)

    def relay_head(h):
        for part in range(2):
            relay((h, part))

    batches = heads // together

    def prepare(i):
        attend_own(i)
        if tree:
            @pl.when(i == jnp.where(me >= 6, 0, batches - 1))
            def _():
                relay(None)
                relay_head(order(0))

    fill_bias(reach)
    loop(prepare, batches)
    arrivals(None, (1, 3) if tree else range(1, reach + 1))
    for slot in range(reach):
        fill_bias(slot)

    def step(i):
        h = order(i)
        if tree:
            @pl.when(i + 1 < heads)
            def _():
                relay_head(order(i + 1))

        for part in range(2):
            arrivals((h, part), (1, 3) if tree else range(1, reach + 1))
        attend(h)

    loop(step)

    def finish(item):
        for kind, cond, off in own_sends:
            @pl.when(cond)
            def _(kind=kind, off=off):
                send(item, kind, 0, lax.rem(me + off, n), off).wait_send()
        if tree:
            @pl.when(me >= 2)
            def _():
                send(item, 3, 2, partner, 1).wait_send()

            @pl.when((me >= 4) & odd)
            def _():
                send(item, 4, 4, me - 1, 3).wait_send()

            if item is not None:
                @pl.when((me >= 6) & (item[0] > 0))
                def _():
                    send(item, 5, 4, me - 2, 2).wait_send()

    finish(None)
    if tree:
        @pl.when(straight)
        def _():
            for item in (None, (0, 0), (0, 1)):
                send(item, 6, 0, me + 2, 2).wait_send()

    def finish_head(h):
        for part in range(2):
            finish((h, part))

    loop(finish_head)


def local(n, queries, keys, values, doc_ids, counts):
    shard_rows, q_heads, width = queries.shape
    heads = keys.shape[1]
    group = q_heads // heads
    reach = min((DOC_MOST + shard_rows - 1) // shard_rows, n - 1)
    rows = shard_rows * group
    out = pl.pallas_call(
        functools.partial(kernel, n, reach, 512),
        out_shape=pltpu.VMEM((shard_rows, heads, group, width), jnp.bfloat16),
        in_specs=[pl.BlockSpec(memory_space=pltpu.HBM)] * 5,
        out_specs=pl.BlockSpec(memory_space=pltpu.VMEM),
        scratch_shapes=[
            pltpu.VMEM((2, shard_rows, heads, width), jnp.bfloat16),
            pltpu.VMEM((heads, 2, reach + 1, shard_rows, width), jnp.bfloat16),
            pltpu.VMEM((heads, shard_rows, group, width), jnp.bfloat16),
            pltpu.VMEM((reach + 1, 1, shard_rows), jnp.int32),
            pltpu.VMEM((rows, (reach + 1) * shard_rows), jnp.float32),
            pltpu.VMEM((heads, rows, width), jnp.float32),
            pltpu.VMEM((heads, rows, width), jnp.float32),
            pltpu.VMEM((heads, rows, width), jnp.float32),
            pltpu.SMEM(counts.shape, jnp.int32),
            pltpu.SemaphoreType.DMA((2,)),
            pltpu.SemaphoreType.DMA((2,)),
            pltpu.SemaphoreType.DMA((heads,)),
            pltpu.SemaphoreType.DMA((heads, 2, 7)),
            pltpu.SemaphoreType.DMA((heads, 2, reach)),
            pltpu.SemaphoreType.DMA((7,)),
            pltpu.SemaphoreType.DMA((reach,)),
        ],
        compiler_params=pltpu.CompilerParams(
            collective_id=0, has_side_effects=True, vmem_limit_bytes=51 << 20
        ),
    )(
        *(
            pltpu.with_memory_space_constraint(x, pltpu.HBM)
            for x in (
                counts,
                queries.reshape(shard_rows, heads, group, width),
                keys,
                values,
                doc_ids.reshape(1, shard_rows),
            )
        )
    )
    return out.reshape(shard_rows, q_heads, width)


def solution(mesh):
    in_specs = (
        P(("dp", "seq"), None, None),
        P(("dp", "seq"), None, None),
        P(("dp", "seq"), None, None),
        P(("dp", "seq")),
        P("dp"),
    )
    out_specs = P(("dp", "seq"), None, None)
    return jax.shard_map(
        functools.partial(local, mesh.shape["seq"]),
        mesh=mesh, in_specs=in_specs, out_specs=out_specs, check_vma=False,
    )
```

```python
import functools
import math

import jax
import jax.numpy as jnp
from jax import lax
from jax.experimental import pallas as pl
from jax.experimental.pallas import tpu as pltpu
from jax.sharding import PartitionSpec as P

DOC_MOST = 512
MESH = pl.DeviceIdType.MESH
NEG = -1e30


def kernel(
    n, reach, tile,
    counts_hbm, q_hbm, k_hbm, v_hbm, docs_hbm, out_ref,
    raw, win, q_vmem, dwin, bias, top_ref, norm_ref, part_ref, counts_ref, small_sem, raw_sem,
    q_sem, send_sem, recv_sem, dsend_sem, drecv_sem,
):
    me = lax.axis_index("seq")
    heads, shard_rows, group, width = q_vmem.shape
    together = math.gcd(heads, 4)
    rows = shard_rows * group
    tree = n == 8 and reach == 4

    even = lax.rem(me, 2) == 0
    odd = jnp.logical_not(even)
    chip_odd = lax.rem(me // 2, 2) == 1
    partner = me + 1 - 2 * lax.rem(me, 2)
    if tree:
        own_sends = [
            (0, jnp.logical_not(chip_odd), 2),
            (1, me < 4, 4),
            (2, even, 1),
        ]
        senders = [
            (odd | (me >= 2), partner),
            (chip_odd | (me == 4) | (me == 5), me - 2),
            (me >= 4, me - 4),
            ((me >= 4) & (me < 6), me + 2),
        ]
        targets = [even | (me >= 2), (me < 4) | jnp.logical_not(chip_odd), me < 4, me >= 6]
        straight = (me == 2) | (me == 3)
        send_shift = jnp.where(me >= 2, 1, 0)
        shift = jnp.where(me >= 6, 1, 0)
    else:
        own_sends = [(off - 1, me + off < n, off) for off in range(1, reach + 1)]
        senders = [(me >= off, me - off) for off in range(1, reach + 1)]
        targets = [me + off < n for off in range(1, reach + 1)]
        send_shift = shift = 0

    barrier = pltpu.get_barrier_semaphore()
    for cond, device in senders:
        @pl.when(cond)
        def _(device=device):
            pl.semaphore_signal(
                barrier, inc=1, device_id={"seq": lax.rem(device + n, n)},
                device_id_type=MESH,
            )

    def loop(body, count=None):
        lax.fori_loop(0, heads if count is None else count, lambda i, c: (body(i), c)[1], 0)

    raw_copies = [
        pltpu.make_async_copy(ref, raw.at[part], raw_sem.at[part])
        for part, ref in enumerate((k_hbm, v_hbm))
    ]
    doc_copy = pltpu.make_async_copy(docs_hbm, dwin.at[reach], small_sem.at[0])
    count_copy = pltpu.make_async_copy(counts_hbm, counts_ref, small_sem.at[1])
    doc_copy.start()
    for copy in raw_copies:
        copy.start()
    count_copy.start()

    def q_copy(h):
        return pltpu.make_async_copy(q_hbm.at[:, h], q_vmem.at[h], q_sem.at[h // together])

    loop(lambda h: q_copy(h).start())

    def recv_index(part, off):
        if not tree:
            return off - 1
        return {1: 3, 2: 0, 3: 3, 4: 1 + part}[off]

    def send(item, kind, from_off, to, to_off):
        if item is None:
            src, dst = dwin.at[reach - from_off], dwin.at[reach - to_off]
            sems = dsend_sem.at[kind], drecv_sem.at[to_off - 1]
        else:
            h, part = item
            src, dst = win.at[h, part, reach - from_off], win.at[h, part, reach - to_off]
            sems = send_sem.at[kind], recv_sem.at[h, recv_index(part, to_off)]
        return pltpu.make_async_remote_copy(
            src_ref=src, dst_ref=dst, send_sem=sems[0], recv_sem=sems[1],
            device_id={"seq": to}, device_id_type=MESH,
        )

    def many(ref, kind=0, recv=(0, 0)):
        return pltpu.make_async_remote_copy(
            src_ref=ref, dst_ref=ref, send_sem=send_sem.at[kind], recv_sem=recv_sem.at[recv],
            device_id={"seq": lax.rem(me + 1, n)}, device_id_type=MESH,
        )

    def wait_block(item, off):
        send(item, 0, 0, lax.rem(me + 1, n), off).wait_recv()

    def wait_both(h, off):
        many(win.at[h, :, reach - off], recv=(h, recv_index(0, off))).wait_recv()

    def start_own(item):
        for kind, cond, off in own_sends:
            @pl.when(cond)
            def _(kind=kind, off=off):
                send(item, kind, 0, lax.rem(me + off, n), off).start()

    doc_copy.wait()
    for part in range(2):
        raw_copies[part].wait()
        win[:, part, reach] = jnp.swapaxes(raw[part], 0, 1)
    pl.semaphore_wait(barrier, sum(jnp.where(cond, 1, 0) for cond in targets))

    start_own(None)
    if tree:
        @pl.when(straight)
        def _():
            for item in (None, (0, 0), (0, 1)):
                send(item, 6, 0, me + 2, 2).start()

    def start_head(i):
        for part in range(2):
            start_own((lax.rem(i + send_shift, heads), part))

    loop(start_head)
    count_copy.wait()

    for off in range(1, reach + 1):
        @pl.when(me < off)
        def _(off=off):
            dwin[reach - off] = jnp.full(dwin.shape[1:], -1, jnp.int32)

            def clear(h):
                win[h, :, reach - off] = jnp.zeros((2, shard_rows, width), win.dtype)

            loop(clear)

    def relay_two(h):
        if h is None:
            wait_block(None, 2)
        else:
            wait_both(h, 2)

        for item in [None] if h is None else [(h, 0), (h, 1)]:
            @pl.when(even)
            def _(item=item):
                send(item, 3, 2, partner, 3).start()

            @pl.when(odd)
            def _(item=item):
                send(item, 3, 2, partner, 1).start()

    def relay_four(item):
        wait_block(item, 4)

        if item is not None:
            @pl.when((me >= 6) & (item[0] > 0))
            def _():
                send(item, 5, 4, me - 2, 2).start()

        @pl.when(odd)
        def _():
            send(item, 4, 4, me - 1, 3).start()

    def relay(h):
        @pl.when(me >= 4)
        def _():
            for item in [None] if h is None else [(h, 0), (h, 1)]:
                relay_four(item)

        @pl.when(me >= 2)
        def _():
            relay_two(h)

    def arrivals(h):
        if h is None:
            for off in (1, 3) if tree else range(1, reach + 1):
                @pl.when(me >= off)
                def _(off=off):
                    wait_block(None, off)
        elif tree:
            @pl.when(me >= 3)
            def _():
                many(win.at[h, :, :2], recv=(h, 3)).wait_recv()

            @pl.when((me == 1) | (me == 2))
            def _():
                many(win.at[h, :, 0], recv=(h, 3)).wait_recv()
        else:
            for off in range(1, reach + 1):
                @pl.when(me >= off)
                def _(off=off):
                    wait_both(h, off)

    lane = lax.broadcasted_iota(jnp.int32, (shard_rows, shard_rows), 1)
    row = lax.broadcasted_iota(jnp.int32, (shard_rows, shard_rows), 0)
    doc_col = jnp.transpose(jnp.broadcast_to(dwin[reach], (shard_rows, shard_rows)))

    def fill_bias(slot):
        off = reach - slot
        count = counts_ref[lax.max(me - off, 0)]
        docs = dwin[slot]
        allowed = (docs == doc_col) & (lane < count)
        if off == 0:
            allowed = allowed & (lane <= row)
        part = jnp.where(allowed, 0.0, NEG).astype(jnp.float32)
        part = jnp.broadcast_to(part[:, None, :], (shard_rows, group, shard_rows))
        bias[:, slot * shard_rows : (slot + 1) * shard_rows] = part.reshape(rows, shard_rows)

    own_count = counts_ref[me]
    factor = math.log2(math.e) / math.sqrt(width)
    remote = reach * shard_rows

    def scores(h, start, keys):
        q = q_vmem[h, start // group : (start + tile) // group].reshape(tile, width)
        return lax.dot_general(
            q, keys, (((1,), (1,)), ((), ())), preferred_element_type=jnp.float32
        )

    def mix(p, values):
        return lax.dot_general(
            p.astype(jnp.bfloat16), values, (((1,), (0,)), ((), ())),
            preferred_element_type=jnp.float32,
        )

    def own_scores(h):
        q = q_vmem[h].reshape(rows, width)
        return lax.dot_general(
            q, win[h, 0, reach], (((1,), (1,)), ((), ())), preferred_element_type=jnp.float32
        )

    def own_weights(h, s):
        x = s * factor + bias[:, remote:]
        top = jnp.max(x, axis=-1, keepdims=True)
        top_ref[h] = jnp.broadcast_to(top, (rows, width))
        return jnp.exp2(x - top)

    def own_mix(h, p):
        ones = jnp.ones((shard_rows, width), jnp.bfloat16)
        o = mix(p, jnp.concatenate([win[h, 1, reach], ones], axis=1))
        part_ref[h] = o[:, :width]
        norm_ref[h] = o[:, width:]

    def attend_own(i):
        hs = [i * together + u for u in range(together)]
        all_q = q_vmem.at[pl.ds(i * together, together)]
        pltpu.make_async_copy(all_q, all_q, q_sem.at[i]).wait()
        s, p = {}, {}
        for k in range(together + 2):
            if k < together:
                s[k] = own_scores(hs[k])
            if 1 <= k <= together:
                p[k - 1] = own_weights(hs[k - 1], s.pop(k - 1))
            if k >= 2:
                own_mix(hs[k - 2], p.pop(k - 2))

    def attend(h):
        keys = win[h, 0, :reach].reshape(remote, width)
        values = win[h, 1, :reach].reshape(remote, width)
        s_next = scores(h, 0, keys)
        for start in range(0, rows, tile):
            at = slice(start, start + tile)
            s = s_next
            if start + tile < rows:
                s_next = scores(h, start + tile, keys)
            x = s * factor + bias[at, :remote]
            own_top = top_ref[h, at]
            top = jnp.maximum(jnp.max(x, axis=-1, keepdims=True), own_top)
            p = jnp.exp2(x - jnp.concatenate([top] * reach, axis=1))
            own = jnp.exp2(own_top - top)
            norm = jnp.sum(p, axis=-1, keepdims=True) + own * norm_ref[h, at]
            o = mix(p, values) + own * part_ref[h, at]
            r = lax.broadcasted_iota(jnp.int32, (tile, width), 0) + start
            o = jnp.where(r < own_count * group, o / norm, 0.0).astype(jnp.bfloat16)
            out_ref[start // group : (start + tile) // group, h] = o.reshape(
                tile // group, group, width
            )

    def order(i):
        return lax.rem(i + shift, heads)

    batches = heads // together

    def prepare(i):
        attend_own(i)
        if tree:
            @pl.when(i == jnp.where(me >= 6, 0, batches - 1))
            def _():
                relay(None)
                relay(order(0))

    fill_bias(reach)
    loop(prepare, batches)
    arrivals(None)
    for slot in range(reach):
        fill_bias(slot)

    def step(i):
        h = order(i)
        if tree:
            @pl.when(i + 1 < heads)
            def _():
                relay(order(i + 1))

        arrivals(h)
        attend(h)

    loop(step)

    ends = [(kind, cond, win.at[:, :, reach]) for kind, cond, _ in own_sends]
    if tree:
        ends += [
            (3, me >= 2, win.at[:, :, reach]),
            (4, (me >= 4) & odd, win.at[:, :, reach]),
            (5, me >= 6, win.at[1:, :, reach]),
            (6, straight, win.at[0, :, reach]),
        ]
    for kind, cond, ref in ends:
        @pl.when(cond)
        def _(kind=kind, ref=ref):
            many(ref, kind=kind).wait_send()
            if kind != 5:
                send(None, kind, 0, lax.rem(me + 1, n), 1).wait_send()


def local(n, queries, keys, values, doc_ids, counts):
    shard_rows, q_heads, width = queries.shape
    heads = keys.shape[1]
    group = q_heads // heads
    reach = min((DOC_MOST + shard_rows - 1) // shard_rows, n - 1)
    rows = shard_rows * group
    out = pl.pallas_call(
        functools.partial(kernel, n, reach, 512),
        out_shape=pltpu.VMEM((shard_rows, heads, group, width), jnp.bfloat16),
        in_specs=[pl.BlockSpec(memory_space=pltpu.HBM)] * 5,
        out_specs=pl.BlockSpec(memory_space=pltpu.VMEM),
        scratch_shapes=[
            pltpu.VMEM((2, shard_rows, heads, width), jnp.bfloat16),
            pltpu.VMEM((heads, 2, reach + 1, shard_rows, width), jnp.bfloat16),
            pltpu.VMEM((heads, shard_rows, group, width), jnp.bfloat16),
            pltpu.VMEM((reach + 1, 1, shard_rows), jnp.int32),
            pltpu.VMEM((rows, (reach + 1) * shard_rows), jnp.float32),
            pltpu.VMEM((heads, rows, width), jnp.float32),
            pltpu.VMEM((heads, rows, width), jnp.float32),
            pltpu.VMEM((heads, rows, width), jnp.float32),
            pltpu.SMEM(counts.shape, jnp.int32),
            pltpu.SemaphoreType.DMA((2,)),
            pltpu.SemaphoreType.DMA((2,)),
            pltpu.SemaphoreType.DMA((heads // math.gcd(heads, 4),)),
            pltpu.SemaphoreType.DMA((7,)),
            pltpu.SemaphoreType.DMA((heads, max(reach, 4))),
            pltpu.SemaphoreType.DMA((7,)),
            pltpu.SemaphoreType.DMA((reach,)),
        ],
        compiler_params=pltpu.CompilerParams(
            collective_id=0, has_side_effects=True, vmem_limit_bytes=51 << 20
        ),
    )(
        *(
            pltpu.with_memory_space_constraint(x, pltpu.HBM)
            for x in (
                counts,
                queries.reshape(shard_rows, heads, group, width),
                keys,
                values,
                doc_ids.reshape(1, shard_rows),
            )
        )
    )
    return out.reshape(shard_rows, q_heads, width)


def solution(mesh):
    in_specs = (
        P(("dp", "seq"), None, None),
        P(("dp", "seq"), None, None),
        P(("dp", "seq"), None, None),
        P(("dp", "seq")),
        P("dp"),
    )
    out_specs = P(("dp", "seq"), None, None)
    return jax.shard_map(
        functools.partial(local, mesh.shape["seq"]),
        mesh=mesh, in_specs=in_specs, out_specs=out_specs, check_vma=False,
    )
```

```python
import functools
import math

import jax
import jax.numpy as jnp
from jax import lax
from jax.experimental import pallas as pl
from jax.experimental.pallas import tpu as pltpu
from jax.sharding import PartitionSpec as P

DOC_MOST = 512
MESH = pl.DeviceIdType.MESH
NEG = -1e30


def kernel(
    n, reach, tile,
    counts_hbm, q_hbm, k_hbm, v_hbm, docs_hbm, out_ref,
    raw, win, q_vmem, dwin, bias, top_ref, norm_ref, part_ref, counts_ref, small_sem, raw_sem,
    q_sem, send_sem, recv_sem, dsend_sem, drecv_sem,
):
    me = lax.axis_index("seq")
    heads, shard_rows, group, width = q_vmem.shape
    together = math.gcd(heads, 4)
    rows = shard_rows * group
    tree = n == 8 and reach == 4

    even = lax.rem(me, 2) == 0
    odd = jnp.logical_not(even)
    chip_odd = lax.rem(me // 2, 2) == 1
    partner = me + 1 - 2 * lax.rem(me, 2)
    if tree:
        straight = (me == 2) | (me == 3)
        last_odd = me == 7
        send_shift = jnp.where(me >= 2, 1, 0)
        shift = jnp.where(me >= 6, 1, 0)
        ahead = jnp.where(last_odd, 1, 0)
        own_sends = [
            (0, jnp.logical_not(chip_odd), jnp.where(even, me + 3, me + 2), jnp.where(even, 1, 2)),
            (1, me < 4, jnp.where(me < 2, me + 4, 7), jnp.where(me == 2, reach + 1, 0)),
            (2, even, me + 1, reach - 1),
        ]
        straight_slot = jnp.where(me == 2, 1, 2)
        senders = [
            (odd | (me >= 2), partner),
            (lax.rem(me, 4) == 3, me - 3),
            (lax.rem(me, 4) == 3, me - 2),
            ((me == 4) | (me == 5), me - 4),
            (last_odd, 2),
            (last_odd, 3),
            (me == 5, 7),
            (me == 5, 2),
            (me == 5, 3),
        ]
        targets = [
            even, odd & (me >= 3), jnp.logical_not(chip_odd), me < 4, last_odd, straight,
        ]
    else:
        own_sends = [
            (off - 1, me + off < n, lax.rem(me + off, n), reach - off)
            for off in range(1, reach + 1)
        ]
        senders = [(me >= off, me - off) for off in range(1, reach + 1)]
        targets = [me + off < n for off in range(1, reach + 1)]
        send_shift = shift = 0

    barrier = pltpu.get_barrier_semaphore()
    for cond, device in senders:
        @pl.when(cond)
        def _(device=device):
            pl.semaphore_signal(
                barrier, inc=1, device_id={"seq": lax.rem(device + n, n)},
                device_id_type=MESH,
            )

    def loop(body, count=None):
        lax.fori_loop(0, heads if count is None else count, lambda i, c: (body(i), c)[1], 0)

    raw_copies = [
        pltpu.make_async_copy(ref, raw.at[part], raw_sem.at[part])
        for part, ref in enumerate((k_hbm, v_hbm))
    ]
    doc_copy = pltpu.make_async_copy(docs_hbm, dwin.at[reach], small_sem.at[0])
    count_copy = pltpu.make_async_copy(counts_hbm, counts_ref, small_sem.at[1])
    doc_copy.start()
    for copy in raw_copies:
        copy.start()
    count_copy.start()

    def q_copy(h):
        return pltpu.make_async_copy(q_hbm.at[:, h], q_vmem.at[h], q_sem.at[h // together])

    loop(lambda h: q_copy(h).start())

    def recv_index(kind, item):
        if not tree:
            return kind
        return {1: 1 if item is None else 1 + item[1], 2: 3, 3: 3, 4: 3}.get(kind, 0)

    def send(item, kind, slot, to, to_slot):
        if item is None:
            src, dst = dwin.at[slot], dwin.at[to_slot]
            sems = dsend_sem.at[kind], drecv_sem.at[recv_index(kind, item)]
        else:
            h, part = item
            src, dst = win.at[h, part, slot], win.at[h, part, to_slot]
            sems = send_sem.at[kind], recv_sem.at[h, recv_index(kind, item)]
        return pltpu.make_async_remote_copy(
            src_ref=src, dst_ref=dst, send_sem=sems[0], recv_sem=sems[1],
            device_id={"seq": to}, device_id_type=MESH,
        )

    def blocks_of(h, count):
        if h is None:
            return dwin.at[:count]
        return win.at[h, :, :count] if count > 1 else win.at[h, :, 0]

    def wait_for(h, index, ref):
        pltpu.make_async_remote_copy(
            src_ref=ref, dst_ref=ref, send_sem=send_sem.at[0],
            recv_sem=drecv_sem.at[index] if h is None else recv_sem.at[h, index],
            device_id={"seq": lax.rem(me + 1, n)}, device_id_type=MESH,
        ).wait_recv()

    def wait_sent(sem, ref):
        pltpu.make_async_remote_copy(
            src_ref=ref, dst_ref=ref, send_sem=sem, recv_sem=recv_sem.at[0, 0],
            device_id={"seq": lax.rem(me + 1, n)}, device_id_type=MESH,
        ).wait_send()

    def items_of(h):
        return [None] if h is None else [(h, 0), (h, 1)]

    def start_own(item):
        for kind, cond, to, slot in own_sends:
            @pl.when(cond)
            def _(kind=kind, to=to, slot=slot):
                send(item, kind, reach, to, slot).start()

    doc_copy.wait()
    for part in range(2):
        raw_copies[part].wait()
        win[:, part, reach] = jnp.swapaxes(raw[part], 0, 1)
    pl.semaphore_wait(barrier, sum(jnp.where(cond, 1, 0) for cond in targets))

    start_own(None)
    if tree:
        @pl.when(straight)
        def _():
            for item in (None, (0, 0), (0, 1)):
                send(item, 6, reach, 5, straight_slot).start()

    def start_head(i):
        for part in range(2):
            start_own((lax.rem(i + send_shift, heads), part))

    loop(start_head)
    count_copy.wait()

    for off in range(1, reach + 1):
        @pl.when(me < off)
        def _(off=off):
            dwin[reach - off] = jnp.full(dwin.shape[1:], -1, jnp.int32)

            def clear(h):
                win[h, :, reach - off] = jnp.zeros((2, shard_rows, width), win.dtype)

            loop(clear)

    def fetch_y(item):
        h = None if item is None else item[0]

        def ref(slots):
            return dwin.at[slots] if item is None else win.at[item[0], item[1], slots]

        @pl.when(last_odd)
        def _():
            wait_for(h, recv_index(1, item), ref(slice(0, 2)))
            if item is not None:
                @pl.when(h > 0)
                def _():
                    send(item, 5, reach + 1, 5, 1).start()
                    send(item, 5, 0, 5, 2).start()

            send(item, 4, reach + 1, 6, 0).start()
            send(item, 4, 0, 6, 1).start()

        @pl.when(me == 5)
        def _():
            wait_for(h, recv_index(1, item), ref(0))
            send(item, 4, 0, 4, 1).start()

    def fetch(h):
        for item in items_of(h):
            fetch_y(item)

        @pl.when(odd & (me >= 3))
        def _():
            wait_for(h, 0, blocks_of(h, 2))
            for item in items_of(h):
                for slot in (1, 2):
                    send(item, 3, slot, me - 1, slot + 1).start()

    def arrivals(h):
        if not tree:
            for off in range(1, reach + 1):
                @pl.when(me >= off)
                def _(off=off):
                    wait_for(h, off - 1, blocks_of(h, 1))
            return

        @pl.when(me == 4)
        def _():
            for item in items_of(h):
                ref = dwin.at[0] if item is None else win.at[item[0], item[1], 0]
                wait_for(h, recv_index(1, item), ref)

        for cond, count in ((odd, 1), (me == 2, 2), (me == 4, 3), (me == 6, 4)):
            @pl.when(cond)
            def _(count=count):
                wait_for(h, 3, blocks_of(h, count))

    lane = lax.broadcasted_iota(jnp.int32, (shard_rows, shard_rows), 1)
    row = lax.broadcasted_iota(jnp.int32, (shard_rows, shard_rows), 0)
    doc_col = jnp.transpose(jnp.broadcast_to(dwin[reach], (shard_rows, shard_rows)))

    def fill_bias(slot):
        off = reach - slot
        count = counts_ref[lax.max(me - off, 0)]
        docs = dwin[slot]
        allowed = (docs == doc_col) & (lane < count)
        if off == 0:
            allowed = allowed & (lane <= row)
        part = jnp.where(allowed, 0.0, NEG).astype(jnp.float32)
        part = jnp.broadcast_to(part[:, None, :], (shard_rows, group, shard_rows))
        bias[:, slot * shard_rows : (slot + 1) * shard_rows] = part.reshape(rows, shard_rows)

    own_count = counts_ref[me]
    factor = math.log2(math.e) / math.sqrt(width)
    remote = reach * shard_rows

    def scores(h, start, keys):
        q = q_vmem[h, start // group : (start + tile) // group].reshape(tile, width)
        return lax.dot_general(
            q, keys, (((1,), (1,)), ((), ())), preferred_element_type=jnp.float32
        )

    def mix(p, values):
        return lax.dot_general(
            p.astype(jnp.bfloat16), values, (((1,), (0,)), ((), ())),
            preferred_element_type=jnp.float32,
        )

    def own_scores(h):
        q = q_vmem[h].reshape(rows, width)
        return lax.dot_general(
            q, win[h, 0, reach], (((1,), (1,)), ((), ())), preferred_element_type=jnp.float32
        )

    def own_weights(h, s):
        x = s * factor + bias[:, remote:]
        top = jnp.max(x, axis=-1, keepdims=True)
        top_ref[h] = jnp.broadcast_to(top, (rows, width))
        return jnp.exp2(x - top)

    def own_mix(h, p):
        ones = jnp.ones((shard_rows, width), jnp.bfloat16)
        o = mix(p, jnp.concatenate([win[h, 1, reach], ones], axis=1))
        part_ref[h] = o[:, :width]
        norm_ref[h] = o[:, width:]

    def attend_own(i):
        hs = [i * together + u for u in range(together)]
        all_q = q_vmem.at[pl.ds(i * together, together)]
        pltpu.make_async_copy(all_q, all_q, q_sem.at[i]).wait()
        s, p = {}, {}
        for k in range(together + 2):
            if k < together:
                s[k] = own_scores(hs[k])
            if 1 <= k <= together:
                p[k - 1] = own_weights(hs[k - 1], s.pop(k - 1))
            if k >= 2:
                own_mix(hs[k - 2], p.pop(k - 2))

    def attend(h):
        keys = win[h, 0, :reach].reshape(remote, width)
        values = win[h, 1, :reach].reshape(remote, width)
        s_next = scores(h, 0, keys)
        for start in range(0, rows, tile):
            at = slice(start, start + tile)
            s = s_next
            if start + tile < rows:
                s_next = scores(h, start + tile, keys)
            x = s * factor + bias[at, :remote]
            own_top = top_ref[h, at]
            top = jnp.maximum(jnp.max(x, axis=-1, keepdims=True), own_top)
            p = jnp.exp2(x - jnp.concatenate([top] * reach, axis=1))
            own = jnp.exp2(own_top - top)
            norm = jnp.sum(p, axis=-1, keepdims=True) + own * norm_ref[h, at]
            o = mix(p, values) + own * part_ref[h, at]
            r = lax.broadcasted_iota(jnp.int32, (tile, width), 0) + start
            o = jnp.where(r < own_count * group, o / norm, 0.0).astype(jnp.bfloat16)
            out_ref[start // group : (start + tile) // group, h] = o.reshape(
                tile // group, group, width
            )

    def order(i):
        return lax.rem(i + shift, heads)

    batches = heads // together

    def prepare(i):
        attend_own(i)
        if tree:
            @pl.when(i == jnp.where(me >= 6, 0, batches - 1))
            def _():
                fetch(None)
                fetch(order(0))

    fill_bias(reach)
    loop(prepare, batches)
    arrivals(None)
    for slot in range(reach):
        fill_bias(slot)

    def step(i):
        h = order(i)
        if tree:
            @pl.when((i + ahead > 0) & (i + ahead < heads))
            def _():
                fetch(order(i + ahead))

        arrivals(h)
        attend(h)

    loop(step)

    ends = [(kind, cond, win.at[:, :, reach], 1) for kind, cond, _, _ in own_sends]
    if tree:
        two = win.at[:, :, :2]
        ends += [
            (3, odd & (me >= 3), two, 2),
            (4, me == 5, win.at[:, :, reach], 1),
            (4, last_odd, two, 2),
            (5, last_odd, win.at[1:, :, :2], 0),
            (6, straight, win.at[0, :, reach], 1),
        ]
    for kind, cond, ref, docs in ends:
        @pl.when(cond)
        def _(kind=kind, ref=ref, docs=docs):
            wait_sent(send_sem.at[kind], ref)
            if docs:
                wait_sent(dsend_sem.at[kind], dwin.at[:docs])


def local(n, queries, keys, values, doc_ids, counts):
    shard_rows, q_heads, width = queries.shape
    heads = keys.shape[1]
    group = q_heads // heads
    reach = min((DOC_MOST + shard_rows - 1) // shard_rows, n - 1)
    rows = shard_rows * group
    out = pl.pallas_call(
        functools.partial(kernel, n, reach, 512),
        out_shape=pltpu.VMEM((shard_rows, heads, group, width), jnp.bfloat16),
        in_specs=[pl.BlockSpec(memory_space=pltpu.HBM)] * 5,
        out_specs=pl.BlockSpec(memory_space=pltpu.VMEM),
        scratch_shapes=[
            pltpu.VMEM((2, shard_rows, heads, width), jnp.bfloat16),
            pltpu.VMEM((heads, 2, reach + 2, shard_rows, width), jnp.bfloat16),
            pltpu.VMEM((heads, shard_rows, group, width), jnp.bfloat16),
            pltpu.VMEM((reach + 2, 1, shard_rows), jnp.int32),
            pltpu.VMEM((rows, (reach + 1) * shard_rows), jnp.float32),
            pltpu.VMEM((heads, rows, width), jnp.float32),
            pltpu.VMEM((heads, rows, width), jnp.float32),
            pltpu.VMEM((heads, rows, width), jnp.float32),
            pltpu.SMEM(counts.shape, jnp.int32),
            pltpu.SemaphoreType.DMA((2,)),
            pltpu.SemaphoreType.DMA((2,)),
            pltpu.SemaphoreType.DMA((heads // math.gcd(heads, 4),)),
            pltpu.SemaphoreType.DMA((7,)),
            pltpu.SemaphoreType.DMA((heads, max(reach, 4))),
            pltpu.SemaphoreType.DMA((7,)),
            pltpu.SemaphoreType.DMA((max(reach, 4),)),
        ],
        compiler_params=pltpu.CompilerParams(
            collective_id=0, has_side_effects=True, vmem_limit_bytes=51 << 20
        ),
    )(
        *(
            pltpu.with_memory_space_constraint(x, pltpu.HBM)
            for x in (
                counts,
                queries.reshape(shard_rows, heads, group, width),
                keys,
                values,
                doc_ids.reshape(1, shard_rows),
            )
        )
    )
    return out.reshape(shard_rows, q_heads, width)


def solution(mesh):
    in_specs = (
        P(("dp", "seq"), None, None),
        P(("dp", "seq"), None, None),
        P(("dp", "seq"), None, None),
        P(("dp", "seq")),
        P("dp"),
    )
    out_specs = P(("dp", "seq"), None, None)
    return jax.shard_map(
        functools.partial(local, mesh.shape["seq"]),
        mesh=mesh, in_specs=in_specs, out_specs=out_specs, check_vma=False,
    )
```

```python
import functools
import math

import jax
import jax.numpy as jnp
from jax import lax
from jax.experimental import pallas as pl
from jax.experimental.pallas import tpu as pltpu
from jax.sharding import PartitionSpec as P

DOC_MOST = 512
MESH = pl.DeviceIdType.MESH
NEG = -1e30


def kernel(
    n, reach, tile,
    counts_hbm, q_hbm, k_hbm, v_hbm, docs_hbm, out_ref,
    raw, win, q_vmem, dwin, bias, weights, top_ref, norm_ref, part_ref, counts_ref, small_sem, raw_sem,
    q_sem, send_sem, recv_sem, block_sem, dsend_sem, drecv_sem,
):
    me = lax.axis_index("seq")
    heads, shard_rows, group, width = q_vmem.shape
    together = math.gcd(heads, 4)
    own = reach + 1
    rows = shard_rows * group
    tree = n == 8 and reach == 4

    even = lax.rem(me, 2) == 0
    odd = jnp.logical_not(even)
    chip_odd = lax.rem(me // 2, 2) == 1
    partner = me + 1 - 2 * lax.rem(me, 2)
    if tree:
        straight = (me == 2) | (me == 3)
        last_odd = me == 7
        send_shift = jnp.where(me >= 2, 1, 0)
        shift = jnp.where(me >= 6, 1, 0)
        ahead = jnp.where(last_odd, 1, 0)
        own_sends = [
            (0, jnp.logical_not(chip_odd), jnp.where(even, me + 3, me + 2), jnp.where(even, 2, 3)),
            (1, me < 4, jnp.where(me < 2, me + 4, 7), jnp.where(me == 2, 0, 1)),
            (2, even, me + 1, reach),
        ]
        straight_slot = jnp.where(me == 2, 2, 3)
        senders = [
            (odd | (me >= 2), partner),
            (lax.rem(me, 4) == 3, me - 3),
            (lax.rem(me, 4) == 3, me - 2),
            ((me == 4) | (me == 5), me - 4),
            (last_odd, 2),
            (last_odd, 3),
            (me == 5, 7),
            (me == 5, 2),
            (me == 5, 3),
        ]
        targets = [
            even, odd & (me >= 3), jnp.logical_not(chip_odd), me < 4, last_odd, straight,
        ]
    else:
        own_sends = [
            (off - 1, me + off < n, lax.rem(me + off, n), own - off)
            for off in range(1, reach + 1)
        ]
        senders = [(me >= off, me - off) for off in range(1, reach + 1)]
        targets = [me + off < n for off in range(1, reach + 1)]
        send_shift = shift = 0

    barrier = pltpu.get_barrier_semaphore()
    for cond, device in senders:
        @pl.when(cond)
        def _(device=device):
            pl.semaphore_signal(
                barrier, inc=1, device_id={"seq": lax.rem(device + n, n)},
                device_id_type=MESH,
            )

    def loop(body, count=None):
        lax.fori_loop(0, heads if count is None else count, lambda i, c: (body(i), c)[1], 0)

    raw_copies = [
        pltpu.make_async_copy(ref, raw.at[part], raw_sem.at[part])
        for part, ref in enumerate((k_hbm, v_hbm))
    ]
    doc_copy = pltpu.make_async_copy(docs_hbm, dwin.at[own], small_sem.at[0])
    count_copy = pltpu.make_async_copy(counts_hbm, counts_ref, small_sem.at[1])
    doc_copy.start()
    for copy in raw_copies:
        copy.start()
    count_copy.start()

    def q_copy(h):
        return pltpu.make_async_copy(q_hbm.at[:, h], q_vmem.at[h], q_sem.at[h // together])

    loop(lambda h: q_copy(h).start())

    both = slice(0, 2)

    def where(item, slot):
        if item is None:
            return dwin.at[slot]
        return win.at[item[0], item[1], slot]

    def recv_index(kind, item):
        if not tree:
            return kind
        if item is None:
            return {1: 1, 2: 4, 3: 3, 4: 3}.get(kind, 0)
        return {1: 2, 3: 4, 4: 4}.get(kind, 0) + item[1]

    def send(item, kind, slot, to, to_slot):
        index = recv_index(kind, item)
        return pltpu.make_async_remote_copy(
            src_ref=where(item, slot), dst_ref=where(item, to_slot),
            send_sem=dsend_sem.at[kind] if item is None else send_sem.at[kind],
            recv_sem=drecv_sem.at[index] if item is None else recv_sem.at[item[0], index],
            device_id={"seq": to}, device_id_type=MESH,
        )

    def send_block():
        return pltpu.make_async_remote_copy(
            src_ref=win.at[:, :, own], dst_ref=win.at[:, :, reach],
            send_sem=send_sem.at[2], recv_sem=block_sem.at[0],
            device_id={"seq": partner}, device_id_type=MESH,
        )

    def wait_for(h, index, ref):
        pltpu.make_async_remote_copy(
            src_ref=ref, dst_ref=ref, send_sem=send_sem.at[0],
            recv_sem=drecv_sem.at[index] if h is None else recv_sem.at[h, index],
            device_id={"seq": lax.rem(me + 1, n)}, device_id_type=MESH,
        ).wait_recv()

    def wait_sent(sem, ref):
        pltpu.make_async_remote_copy(
            src_ref=ref, dst_ref=ref, send_sem=sem, recv_sem=recv_sem.at[0, 0],
            device_id={"seq": lax.rem(me + 1, n)}, device_id_type=MESH,
        ).wait_send()

    def start_own(h):
        for kind, cond, to, slot in own_sends:
            if h is not None and tree and kind == 2:
                continue
            parts = [0, 1] if tree else [both]
            for item in [None] if h is None else [(h, part) for part in parts]:
                @pl.when(cond)
                def _(item=item, kind=kind, to=to, slot=slot):
                    send(item, kind, own, to, slot).start()

    doc_copy.wait()
    for part in range(2):
        raw_copies[part].wait()
        win[:, part, own] = jnp.swapaxes(raw[part], 0, 1)
    pl.semaphore_wait(barrier, sum(jnp.where(cond, 1, 0) for cond in targets))

    start_own(None)
    if tree:
        @pl.when(straight)
        def _():
            for item in (None, (0, 0), (0, 1)):
                send(item, 6, own, 5, straight_slot).start()

    def start_head(i):
        start_own(lax.rem(i + send_shift, heads))

    loop(start_head)
    if tree:
        @pl.when(even)
        def _():
            send_block().start()

    count_copy.wait()

    for off in range(1, reach + 1):
        @pl.when(me < off)
        def _(off=off):
            dwin[own - off] = jnp.full(dwin.shape[1:], -1, jnp.int32)

            def clear(h):
                win[h, :, own - off] = jnp.zeros((2, shard_rows, width), win.dtype)

            loop(clear)

    def fetch_y(item):
        h = None if item is None else item[0]
        index = recv_index(1, item)
        two = slice(0, 2)

        @pl.when(last_odd)
        def _():
            wait_for(h, index, where(item, two))
            if item is not None:
                @pl.when(h > 0)
                def _():
                    send(item, 5, two, 5, slice(2, 4)).start()

            send(item, 4, two, 6, slice(1, 3)).start()

        @pl.when(me == 5)
        def _():
            wait_for(h, index, where(item, 1))
            send(item, 4, 1, 4, 2).start()

    def fetch(item):
        fetch_y(item)

        @pl.when(odd & (me >= 3))
        def _():
            h = None if item is None else item[0]
            wait_for(h, recv_index(0, item), where(item, slice(0, 2)))
            send(item, 3, slice(2, 4), me - 1, slice(3, 5)).start()

    def arrivals(item):
        h = None if item is None else item[0]
        if not tree:
            for off in range(1, reach + 1):
                @pl.when(me >= off)
                def _(off=off):
                    wait_for(h, off - 1, where(item, slice(0, 1)))
            return

        @pl.when(me == 4)
        def _():
            wait_for(h, recv_index(1, item), where(item, 1))

        for cond, count in ((me == 2, 2), (me == 4, 3), (me == 6, 4)):
            @pl.when(cond)
            def _(count=count):
                wait_for(h, recv_index(3, item), where(item, slice(0, count)))

    def arrivals_first():
        arrivals(None)
        if tree:
            @pl.when(odd)
            def _():
                wait_for(None, 4, dwin.at[:1])
                send_block().wait_recv()

    lane = lax.broadcasted_iota(jnp.int32, (shard_rows, shard_rows), 1)
    row = lax.broadcasted_iota(jnp.int32, (shard_rows, shard_rows), 0)
    doc_col = jnp.transpose(jnp.broadcast_to(dwin[own], (shard_rows, shard_rows)))

    def fill_bias(slot):
        off = reach - slot
        count = counts_ref[lax.max(me - off, 0)]
        docs = dwin[slot + 1]
        allowed = (docs == doc_col) & (lane < count)
        if off == 0:
            allowed = allowed & (lane <= row)
        part = jnp.where(allowed, 0.0, NEG).astype(jnp.float32)
        part = jnp.broadcast_to(part[:, None, :], (shard_rows, group, shard_rows))
        bias[:, slot * shard_rows : (slot + 1) * shard_rows] = part.reshape(rows, shard_rows)

    own_count = counts_ref[me]
    factor = math.log2(math.e) / math.sqrt(width)
    remote = reach * shard_rows

    def scores(h, start, keys):
        q = q_vmem[h, start // group : (start + tile) // group].reshape(tile, width)
        return lax.dot_general(
            q, keys, (((1,), (1,)), ((), ())), preferred_element_type=jnp.float32
        )

    def mix(p, values):
        return lax.dot_general(
            p.astype(jnp.bfloat16), values, (((1,), (0,)), ((), ())),
            preferred_element_type=jnp.float32,
        )

    def own_scores(h):
        q = q_vmem[h].reshape(rows, width)
        return lax.dot_general(
            q, win[h, 0, own], (((1,), (1,)), ((), ())), preferred_element_type=jnp.float32
        )

    def own_weights(h, s):
        x = s * factor + bias[:, remote:]
        top = jnp.max(x, axis=-1, keepdims=True)
        top_ref[h] = jnp.broadcast_to(top, (rows, width))
        return jnp.exp2(x - top)

    def own_mix(h, p):
        ones = jnp.ones((shard_rows, width), jnp.bfloat16)
        o = mix(p, jnp.concatenate([win[h, 1, own], ones], axis=1))
        part_ref[h] = o[:, :width]
        norm_ref[h] = o[:, width:]

    def attend_own(i):
        hs = [i * together + u for u in range(together)]
        all_q = q_vmem.at[pl.ds(i * together, together)]
        pltpu.make_async_copy(all_q, all_q, q_sem.at[i]).wait()
        s, p = {}, {}
        for k in range(together + 2):
            if k < together:
                s[k] = own_scores(hs[k])
            if 1 <= k <= together:
                p[k - 1] = own_weights(hs[k - 1], s.pop(k - 1))
            if k >= 2:
                own_mix(hs[k - 2], p.pop(k - 2))

    def attend_keys(h):
        keys = win[h, 0, 1:own].reshape(remote, width)
        s_next = scores(h, 0, keys)
        for start in range(0, rows, tile):
            at = slice(start, start + tile)
            s = s_next
            if start + tile < rows:
                s_next = scores(h, start + tile, keys)
            x = s * factor + bias[at, :remote]
            own_top = top_ref[h, at]
            top = jnp.maximum(jnp.max(x, axis=-1, keepdims=True), own_top)
            p = jnp.exp2(x - jnp.concatenate([top] * reach, axis=1))
            scale = jnp.exp2(own_top - top)
            weights[at] = p.astype(jnp.bfloat16)
            top_ref[h, at] = scale
            norm_ref[h, at] = jnp.sum(p, axis=-1, keepdims=True) + scale * norm_ref[h, at]

    def attend_values(h):
        values = win[h, 1, 1:own].reshape(remote, width)
        for start in range(0, rows, tile):
            at = slice(start, start + tile)
            o = mix(weights[at], values) + top_ref[h, at] * part_ref[h, at]
            r = lax.broadcasted_iota(jnp.int32, (tile, width), 0) + start
            o = jnp.where(r < own_count * group, o / norm_ref[h, at], 0.0).astype(jnp.bfloat16)
            out_ref[start // group : (start + tile) // group, h] = o.reshape(
                tile // group, group, width
            )

    def order(i):
        return lax.rem(i + shift, heads)

    fill_bias(reach)
    loop(attend_own, heads // together)
    if tree:
        for item in (None, (order(0), 0), (order(0), 1)):
            fetch(item)
    arrivals_first()
    for slot in range(reach):
        fill_bias(slot)

    def step(i):
        h = order(i)
        for part, attend in enumerate((attend_keys, attend_values)):
            if tree:
                @pl.when((i + ahead > 0) & (i + ahead < heads))
                def _(part=part):
                    fetch((order(i + ahead), part))

            if tree:
                arrivals((h, part))
            elif part == 0:
                arrivals((h, both))
            attend(h)

    loop(step)

    one, two = win.at[:, :, own], win.at[:, :, :2]
    ends = [(kind, cond, one, 1) for kind, cond, _, _ in own_sends]
    if tree:
        ends += [
            (3, odd & (me >= 3), two, 2),
            (4, me == 5, one, 1),
            (4, last_odd, two, 2),
            (5, last_odd, win.at[1:, :, :2], 0),
            (6, straight, win.at[0, :, own], 1),
        ]
    for kind, cond, ref, docs in ends:
        @pl.when(cond)
        def _(kind=kind, ref=ref, docs=docs):
            wait_sent(send_sem.at[kind], ref)
            if docs:
                wait_sent(dsend_sem.at[kind], dwin.at[:docs])


def local(n, queries, keys, values, doc_ids, counts):
    shard_rows, q_heads, width = queries.shape
    heads = keys.shape[1]
    group = q_heads // heads
    reach = min((DOC_MOST + shard_rows - 1) // shard_rows, n - 1)
    rows = shard_rows * group
    out = pl.pallas_call(
        functools.partial(kernel, n, reach, 512),
        out_shape=pltpu.VMEM((shard_rows, heads, group, width), jnp.bfloat16),
        in_specs=[pl.BlockSpec(memory_space=pltpu.HBM)] * 5,
        out_specs=pl.BlockSpec(memory_space=pltpu.VMEM),
        scratch_shapes=[
            pltpu.VMEM((2, shard_rows, heads, width), jnp.bfloat16),
            pltpu.VMEM((heads, 2, reach + 2, shard_rows, width), jnp.bfloat16),
            pltpu.VMEM((heads, shard_rows, group, width), jnp.bfloat16),
            pltpu.VMEM((reach + 2, 1, shard_rows), jnp.int32),
            pltpu.VMEM((rows, (reach + 1) * shard_rows), jnp.float32),
            pltpu.VMEM((rows, reach * shard_rows), jnp.bfloat16),
            pltpu.VMEM((heads, rows, width), jnp.float32),
            pltpu.VMEM((heads, rows, width), jnp.float32),
            pltpu.VMEM((heads, rows, width), jnp.float32),
            pltpu.SMEM(counts.shape, jnp.int32),
            pltpu.SemaphoreType.DMA((2,)),
            pltpu.SemaphoreType.DMA((2,)),
            pltpu.SemaphoreType.DMA((heads // math.gcd(heads, 4),)),
            pltpu.SemaphoreType.DMA((7,)),
            pltpu.SemaphoreType.DMA((heads, max(reach, 6))),
            pltpu.SemaphoreType.DMA((1,)),
            pltpu.SemaphoreType.DMA((7,)),
            pltpu.SemaphoreType.DMA((max(reach, 5),)),
        ],
        compiler_params=pltpu.CompilerParams(
            collective_id=0, has_side_effects=True, vmem_limit_bytes=51 << 20
        ),
    )(
        *(
            pltpu.with_memory_space_constraint(x, pltpu.HBM)
            for x in (
                counts,
                queries.reshape(shard_rows, heads, group, width),
                keys,
                values,
                doc_ids.reshape(1, shard_rows),
            )
        )
    )
    return out.reshape(shard_rows, q_heads, width)


def solution(mesh):
    in_specs = (
        P(("dp", "seq"), None, None),
        P(("dp", "seq"), None, None),
        P(("dp", "seq"), None, None),
        P(("dp", "seq")),
        P("dp"),
    )
    out_specs = P(("dp", "seq"), None, None)
    return jax.shard_map(
        functools.partial(local, mesh.shape["seq"]),
        mesh=mesh, in_specs=in_specs, out_specs=out_specs, check_vma=False,
    )
```

```python
import functools
import math

import jax
import jax.numpy as jnp
from jax import lax
from jax.experimental import pallas as pl
from jax.experimental.pallas import tpu as pltpu
from jax.sharding import PartitionSpec as P

DOC_MOST = 512
MESH = pl.DeviceIdType.MESH
NEG = -1e30


def kernel(
    n, reach, tile,
    counts_hbm, q_hbm, k_hbm, v_hbm, docs_hbm, out_ref,
    raw, win, q_vmem, dwin, bias, weights, top_ref, norm_ref, part_ref, counts_ref, small_sem, raw_sem,
    q_sem, send_sem, recv_sem, block_sem, dsend_sem, drecv_sem,
):
    me = lax.axis_index("seq")
    heads, shard_rows, group, width = q_vmem.shape
    together = math.gcd(heads, 4)
    own = reach + 1
    rows = shard_rows * group
    tree = n == 8 and reach == 4

    even = lax.rem(me, 2) == 0
    odd = jnp.logical_not(even)
    chip_odd = lax.rem(me // 2, 2) == 1
    partner = me + 1 - 2 * lax.rem(me, 2)
    if tree:
        straight = (me == 2) | (me == 3)
        last_odd = me == 7
        send_shift = jnp.where(me >= 2, 1, 0)
        shift = jnp.where(me >= 6, 1, 0)
        ahead = jnp.where(last_odd, 1, 0)
        own_sends = [
            (0, jnp.logical_not(chip_odd), jnp.where(even, me + 3, me + 2), jnp.where(even, 2, 3)),
            (1, me < 4, jnp.where(me < 2, me + 4, 7), jnp.where(me == 2, 0, 1)),
            (2, even, me + 1, reach),
        ]
        straight_slot = jnp.where(me == 2, 2, 3)
        senders = [
            (odd | (me >= 2), partner),
            (lax.rem(me, 4) == 3, me - 3),
            (lax.rem(me, 4) == 3, me - 2),
            ((me == 4) | (me == 5), me - 4),
            (last_odd, 2),
            (last_odd, 3),
            (me == 5, 7),
            (me == 5, 2),
            (me == 5, 3),
        ]
        targets = [
            even, odd & (me >= 3), jnp.logical_not(chip_odd), me < 4, last_odd, straight,
        ]
    else:
        own_sends = [
            (off - 1, me + off < n, lax.rem(me + off, n), own - off)
            for off in range(1, reach + 1)
        ]
        senders = [(me >= off, me - off) for off in range(1, reach + 1)]
        targets = [me + off < n for off in range(1, reach + 1)]
        send_shift = shift = 0

    barrier = pltpu.get_barrier_semaphore()
    for cond, device in senders:
        @pl.when(cond)
        def _(device=device):
            pl.semaphore_signal(
                barrier, inc=1, device_id={"seq": lax.rem(device + n, n)},
                device_id_type=MESH,
            )

    def loop(body, count=None):
        lax.fori_loop(0, heads if count is None else count, lambda i, c: (body(i), c)[1], 0)

    raw_copies = [
        pltpu.make_async_copy(ref, raw.at[part], raw_sem.at[0])
        for part, ref in enumerate((k_hbm, v_hbm))
    ]
    doc_copy = pltpu.make_async_copy(docs_hbm, dwin.at[own], small_sem.at[0])
    count_copy = pltpu.make_async_copy(counts_hbm, counts_ref, small_sem.at[1])
    doc_copy.start()
    for copy in raw_copies:
        copy.start()
    count_copy.start()

    def q_copy(h):
        return pltpu.make_async_copy(q_hbm.at[:, h], q_vmem.at[h], q_sem.at[0])

    loop(lambda h: q_copy(h).start())

    both = slice(0, 2)

    def where(item, slot):
        if item is None:
            return dwin.at[slot]
        return win.at[item[0], item[1], slot]

    def recv_index(kind, item):
        if not tree:
            return kind
        if item is None:
            return {1: 1, 2: 2}.get(kind, 0)
        return (2 if kind == 1 else 0) + item[1]

    def send(item, kind, slot, to, to_slot):
        index = recv_index(kind, item)
        return pltpu.make_async_remote_copy(
            src_ref=where(item, slot), dst_ref=where(item, to_slot),
            send_sem=dsend_sem.at[0] if item is None else send_sem.at[kind],
            recv_sem=drecv_sem.at[index] if item is None else recv_sem.at[item[0], index],
            device_id={"seq": to}, device_id_type=MESH,
        )

    def send_block():
        return pltpu.make_async_remote_copy(
            src_ref=win.at[:, :, own], dst_ref=win.at[:, :, reach],
            send_sem=send_sem.at[2], recv_sem=block_sem.at[0],
            device_id={"seq": partner}, device_id_type=MESH,
        )

    def wait_for(h, index, ref):
        pltpu.make_async_remote_copy(
            src_ref=ref, dst_ref=ref, send_sem=send_sem.at[0],
            recv_sem=drecv_sem.at[index] if h is None else recv_sem.at[h, index],
            device_id={"seq": lax.rem(me + 1, n)}, device_id_type=MESH,
        ).wait_recv()

    def wait_sent(sem, ref):
        pltpu.make_async_remote_copy(
            src_ref=ref, dst_ref=ref, send_sem=sem, recv_sem=recv_sem.at[0, 0],
            device_id={"seq": lax.rem(me + 1, n)}, device_id_type=MESH,
        ).wait_send()

    def start_own(h):
        for kind, cond, to, slot in own_sends:
            if h is not None and tree and kind == 2:
                continue
            parts = [0, 1] if tree else [both]
            for item in [None] if h is None else [(h, part) for part in parts]:
                @pl.when(cond)
                def _(item=item, kind=kind, to=to, slot=slot):
                    send(item, kind, own, to, slot).start()

    doc_copy.wait()
    pltpu.make_async_copy(raw, raw, raw_sem.at[0]).wait()
    for part in range(2):
        win[:, part, own] = jnp.swapaxes(raw[part], 0, 1)
    pl.semaphore_wait(barrier, sum(jnp.where(cond, 1, 0) for cond in targets))

    start_own(None)
    if tree:
        @pl.when(straight)
        def _():
            for item in (None, (0, 0), (0, 1)):
                send(item, 6, own, 5, straight_slot).start()

    def start_head(i):
        start_own(lax.rem(i + send_shift, heads))

    loop(start_head)
    if tree:
        @pl.when(even)
        def _():
            send_block().start()

    count_copy.wait()

    for off in range(1, reach + 1):
        @pl.when(me < off)
        def _(off=off):
            dwin[own - off] = jnp.full(dwin.shape[1:], -1, jnp.int32)

            def clear(h):
                win[h, :, own - off] = jnp.zeros((2, shard_rows, width), win.dtype)

            loop(clear)

    def fetch_y(item):
        h = None if item is None else item[0]
        index = recv_index(1, item)
        two = slice(0, 2)

        @pl.when(last_odd)
        def _():
            wait_for(h, index, where(item, two))
            if item is not None:
                @pl.when(h > 0)
                def _():
                    send(item, 5, two, 5, slice(2, 4)).start()

            send(item, 4, two, 6, slice(1, 3)).start()

        @pl.when(me == 5)
        def _():
            wait_for(h, index, where(item, 1))
            send(item, 4, 1, 4, 2).start()

    def fetch(item):
        fetch_y(item)

        @pl.when(odd & (me >= 3))
        def _():
            h = None if item is None else item[0]
            wait_for(h, recv_index(0, item), where(item, slice(0, 2)))
            send(item, 3, slice(2, 4), me - 1, slice(3, 5)).start()

    def arrivals(item):
        h = None if item is None else item[0]
        if not tree:
            for off in range(1, reach + 1):
                @pl.when(me >= off)
                def _(off=off):
                    wait_for(h, off - 1, where(item, slice(0, 1)))
            return

        @pl.when(me == 4)
        def _():
            wait_for(h, recv_index(1, item), where(item, 1))

        for cond, count in ((me == 2, 2), (me == 4, 3), (me == 6, 4)):
            @pl.when(cond)
            def _(count=count):
                wait_for(h, recv_index(3, item), where(item, slice(0, count)))

    def arrivals_first():
        arrivals(None)
        if tree:
            @pl.when(odd)
            def _():
                wait_for(None, 2, dwin.at[:1])
                send_block().wait_recv()

    lane = lax.broadcasted_iota(jnp.int32, (shard_rows, shard_rows), 1)
    row = lax.broadcasted_iota(jnp.int32, (shard_rows, shard_rows), 0)
    doc_col = jnp.transpose(jnp.broadcast_to(dwin[own], (shard_rows, shard_rows)))

    def fill_bias(slot):
        off = reach - slot
        count = counts_ref[lax.max(me - off, 0)]
        docs = dwin[slot + 1]
        allowed = (docs == doc_col) & (lane < count)
        if off == 0:
            allowed = allowed & (lane <= row)
        part = jnp.where(allowed, 0.0, NEG).astype(jnp.float32)
        part = jnp.broadcast_to(part[:, None, :], (shard_rows, group, shard_rows))
        bias[:, slot * shard_rows : (slot + 1) * shard_rows] = part.reshape(rows, shard_rows)

    own_count = counts_ref[me]
    factor = math.log2(math.e) / math.sqrt(width)
    remote = reach * shard_rows

    def scores(h, start, keys):
        q = q_vmem[h, start // group : (start + tile) // group].reshape(tile, width)
        return lax.dot_general(
            q, keys, (((1,), (1,)), ((), ())), preferred_element_type=jnp.float32
        )

    def mix(p, values):
        return lax.dot_general(
            p.astype(jnp.bfloat16), values, (((1,), (0,)), ((), ())),
            preferred_element_type=jnp.float32,
        )

    def own_scores(h):
        q = q_vmem[h].reshape(rows, width)
        return lax.dot_general(
            q, win[h, 0, own], (((1,), (1,)), ((), ())), preferred_element_type=jnp.float32
        )

    def own_weights(h, s):
        x = s * factor + bias[:, remote:]
        top = jnp.max(x, axis=-1, keepdims=True)
        top_ref[h] = jnp.broadcast_to(top, (rows, width))
        return jnp.exp2(x - top)

    def own_mix(h, p):
        ones = jnp.ones((shard_rows, width), jnp.bfloat16)
        o = mix(p, jnp.concatenate([win[h, 1, own], ones], axis=1))
        part_ref[h] = o[:, :width]
        norm_ref[h] = o[:, width:]

    def attend_own(i):
        hs = [i * together + u for u in range(together)]
        s, p = {}, {}
        for k in range(together + 2):
            if k < together:
                s[k] = own_scores(hs[k])
            if 1 <= k <= together:
                p[k - 1] = own_weights(hs[k - 1], s.pop(k - 1))
            if k >= 2:
                own_mix(hs[k - 2], p.pop(k - 2))

    def attend_keys(h):
        keys = win[h, 0, 1:own].reshape(remote, width)
        s_next = scores(h, 0, keys)
        for start in range(0, rows, tile):
            at = slice(start, start + tile)
            s = s_next
            if start + tile < rows:
                s_next = scores(h, start + tile, keys)
            x = s * factor + bias[at, :remote]
            own_top = top_ref[h, at]
            top = jnp.maximum(jnp.max(x, axis=-1, keepdims=True), own_top)
            p = jnp.exp2(x - jnp.concatenate([top] * reach, axis=1))
            scale = jnp.exp2(own_top - top)
            weights[at] = p.astype(jnp.bfloat16)
            top_ref[h, at] = scale
            norm_ref[h, at] = jnp.sum(p, axis=-1, keepdims=True) + scale * norm_ref[h, at]

    def attend_values(h):
        values = win[h, 1, 1:own].reshape(remote, width)
        for start in range(0, rows, tile):
            at = slice(start, start + tile)
            o = mix(weights[at], values) + top_ref[h, at] * part_ref[h, at]
            r = lax.broadcasted_iota(jnp.int32, (tile, width), 0) + start
            o = jnp.where(r < own_count * group, o / norm_ref[h, at], 0.0).astype(jnp.bfloat16)
            out_ref[start // group : (start + tile) // group, h] = o.reshape(
                tile // group, group, width
            )

    def order(i):
        return lax.rem(i + shift, heads)

    fill_bias(reach)
    pltpu.make_async_copy(q_vmem, q_vmem, q_sem.at[0]).wait()
    loop(attend_own, heads // together)
    if tree:
        for item in (None, (order(0), 0), (order(0), 1)):
            fetch(item)
    arrivals_first()
    for slot in range(reach):
        fill_bias(slot)

    def step(i):
        h = order(i)
        for part, attend in enumerate((attend_keys, attend_values)):
            if tree:
                @pl.when((i + ahead > 0) & (i + ahead < heads))
                def _(part=part):
                    fetch((order(i + ahead), part))

            if tree:
                arrivals((h, part))
            elif part == 0:
                arrivals((h, both))
            attend(h)

    loop(step)

    one, two = win.at[:, :, own], win.at[:, :, :2]
    ends = [(kind, cond, one, 1) for kind, cond, _, _ in own_sends]
    if tree:
        ends += [
            (3, odd & (me >= 3), two, 2),
            (4, me == 5, one, 1),
            (4, last_odd, two, 2),
            (5, last_odd, win.at[1:, :, :2], 0),
            (6, straight, win.at[0, :, own], 1),
        ]
    for kind, cond, ref, _ in ends:
        @pl.when(cond)
        def _(kind=kind, ref=ref):
            wait_sent(send_sem.at[kind], ref)

    sent = sum(jnp.where(cond, docs, 0) for _, cond, _, docs in ends)
    for count in range(1, max(reach, 4) + 1):
        @pl.when(sent == count)
        def _(count=count):
            wait_sent(dsend_sem.at[0], dwin.at[:count])


def local(n, queries, keys, values, doc_ids, counts):
    shard_rows, q_heads, width = queries.shape
    heads = keys.shape[1]
    group = q_heads // heads
    reach = min((DOC_MOST + shard_rows - 1) // shard_rows, n - 1)
    rows = shard_rows * group
    out = pl.pallas_call(
        functools.partial(kernel, n, reach, 512),
        out_shape=pltpu.VMEM((shard_rows, heads, group, width), jnp.bfloat16),
        in_specs=[pl.BlockSpec(memory_space=pltpu.HBM)] * 5,
        out_specs=pl.BlockSpec(memory_space=pltpu.VMEM),
        scratch_shapes=[
            pltpu.VMEM((2, shard_rows, heads, width), jnp.bfloat16),
            pltpu.VMEM((heads, 2, reach + 2, shard_rows, width), jnp.bfloat16),
            pltpu.VMEM((heads, shard_rows, group, width), jnp.bfloat16),
            pltpu.VMEM((reach + 2, 1, shard_rows), jnp.int32),
            pltpu.VMEM((rows, (reach + 1) * shard_rows), jnp.float32),
            pltpu.VMEM((rows, reach * shard_rows), jnp.bfloat16),
            pltpu.VMEM((heads, rows, width), jnp.float32),
            pltpu.VMEM((heads, rows, width), jnp.float32),
            pltpu.VMEM((heads, rows, width), jnp.float32),
            pltpu.SMEM(counts.shape, jnp.int32),
            pltpu.SemaphoreType.DMA((2,)),
            pltpu.SemaphoreType.DMA((1,)),
            pltpu.SemaphoreType.DMA((1,)),
            pltpu.SemaphoreType.DMA((7,)),
            pltpu.SemaphoreType.DMA((heads, max(reach, 4))),
            pltpu.SemaphoreType.DMA((1,)),
            pltpu.SemaphoreType.DMA((1,)),
            pltpu.SemaphoreType.DMA((max(reach, 3),)),
        ],
        compiler_params=pltpu.CompilerParams(
            collective_id=0, has_side_effects=True, vmem_limit_bytes=51 << 20
        ),
    )(
        *(
            pltpu.with_memory_space_constraint(x, pltpu.HBM)
            for x in (
                counts,
                queries.reshape(shard_rows, heads, group, width),
                keys,
                values,
                doc_ids.reshape(1, shard_rows),
            )
        )
    )
    return out.reshape(shard_rows, q_heads, width)


def solution(mesh):
    in_specs = (
        P(("dp", "seq"), None, None),
        P(("dp", "seq"), None, None),
        P(("dp", "seq"), None, None),
        P(("dp", "seq")),
        P("dp"),
    )
    out_specs = P(("dp", "seq"), None, None)
    return jax.shard_map(
        functools.partial(local, mesh.shape["seq"]),
        mesh=mesh, in_specs=in_specs, out_specs=out_specs, check_vma=False,
    )
```

```python
import functools
import math

import jax
import jax.numpy as jnp
from jax import lax
from jax.experimental import pallas as pl
from jax.experimental.pallas import tpu as pltpu
from jax.sharding import PartitionSpec as P

DOC_MOST = 512
MESH = pl.DeviceIdType.MESH
NEG = -1e30


def mix(p, values):
    return lax.dot_general(
        p.astype(jnp.bfloat16), values, (((1,), (0,)), ((), ())),
        preferred_element_type=jnp.float32,
    )


def mixed(weights, values, scale, part, norm):
    return ((mix(weights, values) + scale * part) / norm).astype(jnp.bfloat16)


def first_head(n, tree):
    return jnp.where(lax.axis_index("seq") >= 6, 1, 0) if tree else 0


def finish_kernel(
    n, tree, tile,
    mixed_ref, weights, top_ref, norm_ref, part_ref, values, out_hbm, last, sem,
):
    rows, remote = weights.shape
    shard_rows, heads, group, width = mixed_ref.shape
    first = first_head(n, tree)

    def copy(i, c):
        h = lax.rem(i + first, heads)
        pltpu.make_async_copy(mixed_ref.at[:, h], out_hbm.at[:, h], sem.at[0]).start()
        return c

    lax.fori_loop(0, heads - 1, copy, 0)
    h = lax.rem(heads - 1 + first, heads)
    for start in range(0, rows, tile):
        at = slice(start, start + tile)
        places = slice(start // group, (start + tile) // group)
        last[places] = mixed(
            weights[at], values[...], top_ref[h, at], part_ref[h, at], norm_ref[h, at],
        ).reshape(tile // group, group, width)
        pltpu.make_async_copy(last.at[places], out_hbm.at[places, h], sem.at[1]).start()
    rest = mixed_ref.at[:, 1:]
    pltpu.make_async_copy(rest, rest, sem.at[0]).wait()
    pltpu.make_async_copy(last, last, sem.at[1]).wait()


def kernel(
    n, reach, tile,
    counts_hbm, q_hbm, k_hbm, v_hbm, docs_hbm,
    out_ref, weights, top_ref, norm_ref, part_ref, last_values,
    raw, win, q_vmem, dwin, bias, counts_ref, small_sem, raw_sem,
    q_sem, send_sem, recv_sem, block_sem, dsend_sem, drecv_sem,
):
    me = lax.axis_index("seq")
    heads, shard_rows, group, width = q_vmem.shape
    together = math.gcd(heads, 4)
    own = reach + 1
    rows = shard_rows * group
    tree = n == 8 and reach == 4

    even = lax.rem(me, 2) == 0
    odd = jnp.logical_not(even)
    chip_odd = lax.rem(me // 2, 2) == 1
    partner = me + 1 - 2 * lax.rem(me, 2)
    if tree:
        straight = (me == 2) | (me == 3)
        last_odd = me == 7
        send_shift = jnp.where(me >= 2, 1, 0)
        ahead = jnp.where(last_odd, 1, 0)
        own_sends = [
            (0, jnp.logical_not(chip_odd), jnp.where(even, me + 3, me + 2), jnp.where(even, 2, 3)),
            (1, me < 4, jnp.where(me < 2, me + 4, 7), jnp.where(me == 2, 0, 1)),
            (2, even, me + 1, reach),
        ]
        straight_slot = jnp.where(me == 2, 2, 3)
        senders = [
            (odd | (me >= 2), partner),
            (lax.rem(me, 4) == 3, me - 3),
            (lax.rem(me, 4) == 3, me - 2),
            ((me == 4) | (me == 5), me - 4),
            (last_odd, 2),
            (last_odd, 3),
            (me == 5, 7),
            (me == 5, 2),
            (me == 5, 3),
        ]
        targets = [
            even, odd & (me >= 3), jnp.logical_not(chip_odd), me < 4, last_odd, straight,
        ]
    else:
        own_sends = [
            (off - 1, me + off < n, lax.rem(me + off, n), own - off)
            for off in range(1, reach + 1)
        ]
        senders = [(me >= off, me - off) for off in range(1, reach + 1)]
        targets = [me + off < n for off in range(1, reach + 1)]
        send_shift = 0

    barrier = pltpu.get_barrier_semaphore()
    for cond, device in senders:
        @pl.when(cond)
        def _(device=device):
            pl.semaphore_signal(
                barrier, inc=1, device_id={"seq": lax.rem(device + n, n)},
                device_id_type=MESH,
            )

    def loop(body, count=None):
        lax.fori_loop(0, heads if count is None else count, lambda i, c: (body(i), c)[1], 0)

    raw_copies = [
        pltpu.make_async_copy(ref, raw.at[part], raw_sem.at[0])
        for part, ref in enumerate((k_hbm, v_hbm))
    ]
    doc_copy = pltpu.make_async_copy(docs_hbm, dwin.at[own], small_sem.at[0])
    count_copy = pltpu.make_async_copy(counts_hbm, counts_ref, small_sem.at[1])
    doc_copy.start()
    for copy in raw_copies:
        copy.start()
    count_copy.start()

    def q_copy(h):
        return pltpu.make_async_copy(q_hbm.at[:, h], q_vmem.at[h], q_sem.at[0])

    loop(lambda h: q_copy(h).start())

    both = slice(0, 2)

    def where(item, slot):
        if item is None:
            return dwin.at[slot]
        return win.at[item[0], item[1], slot]

    def recv_index(kind, item):
        if not tree:
            return kind
        if item is None:
            return {1: 1, 2: 2}.get(kind, 0)
        return (2 if kind == 1 else 0) + item[1]

    def send(item, kind, slot, to, to_slot):
        index = recv_index(kind, item)
        return pltpu.make_async_remote_copy(
            src_ref=where(item, slot), dst_ref=where(item, to_slot),
            send_sem=dsend_sem.at[0] if item is None else send_sem.at[kind],
            recv_sem=drecv_sem.at[index] if item is None else recv_sem.at[item[0], index],
            device_id={"seq": to}, device_id_type=MESH,
        )

    def send_block():
        return pltpu.make_async_remote_copy(
            src_ref=win.at[:, :, own], dst_ref=win.at[:, :, reach],
            send_sem=send_sem.at[2], recv_sem=block_sem.at[0],
            device_id={"seq": partner}, device_id_type=MESH,
        )

    def wait_for(h, index, ref):
        pltpu.make_async_remote_copy(
            src_ref=ref, dst_ref=ref, send_sem=send_sem.at[0],
            recv_sem=drecv_sem.at[index] if h is None else recv_sem.at[h, index],
            device_id={"seq": lax.rem(me + 1, n)}, device_id_type=MESH,
        ).wait_recv()

    def wait_sent(sem, ref):
        pltpu.make_async_remote_copy(
            src_ref=ref, dst_ref=ref, send_sem=sem, recv_sem=recv_sem.at[0, 0],
            device_id={"seq": lax.rem(me + 1, n)}, device_id_type=MESH,
        ).wait_send()

    def start_own(h):
        for kind, cond, to, slot in own_sends:
            if h is not None and tree and kind == 2:
                continue
            parts = [0, 1] if tree else [both]
            for item in [None] if h is None else [(h, part) for part in parts]:
                @pl.when(cond)
                def _(item=item, kind=kind, to=to, slot=slot):
                    send(item, kind, own, to, slot).start()

    doc_copy.wait()
    pltpu.make_async_copy(raw, raw, raw_sem.at[0]).wait()
    for part in range(2):
        win[:, part, own] = jnp.swapaxes(raw[part], 0, 1)
    pl.semaphore_wait(barrier, sum(jnp.where(cond, 1, 0) for cond in targets))

    start_own(None)
    if tree:
        @pl.when(straight)
        def _():
            for item in (None, (0, 0), (0, 1)):
                send(item, 6, own, 5, straight_slot).start()

    def start_head(i):
        start_own(lax.rem(i + send_shift, heads))

    loop(start_head)
    if tree:
        @pl.when(even)
        def _():
            send_block().start()

    count_copy.wait()

    for off in range(1, reach + 1):
        @pl.when(me < off)
        def _(off=off):
            dwin[own - off] = jnp.full(dwin.shape[1:], -1, jnp.int32)

            def clear(h):
                win[h, :, own - off] = jnp.zeros((2, shard_rows, width), win.dtype)

            loop(clear)

    def fetch_y(item):
        h = None if item is None else item[0]
        index = recv_index(1, item)
        two = slice(0, 2)

        @pl.when(last_odd)
        def _():
            wait_for(h, index, where(item, two))
            if item is not None:
                @pl.when(h > 0)
                def _():
                    send(item, 5, two, 5, slice(2, 4)).start()

            send(item, 4, two, 6, slice(1, 3)).start()

        @pl.when(me == 5)
        def _():
            wait_for(h, index, where(item, 1))
            send(item, 4, 1, 4, 2).start()

    def fetch(item):
        fetch_y(item)

        @pl.when(odd & (me >= 3))
        def _():
            h = None if item is None else item[0]
            wait_for(h, recv_index(0, item), where(item, slice(0, 2)))
            send(item, 3, slice(2, 4), me - 1, slice(3, 5)).start()

    def arrivals(item):
        h = None if item is None else item[0]
        if not tree:
            for off in range(1, reach + 1):
                @pl.when(me >= off)
                def _(off=off):
                    wait_for(h, off - 1, where(item, slice(0, 1)))
            return

        @pl.when(me == 4)
        def _():
            wait_for(h, recv_index(1, item), where(item, 1))

        for cond, count in ((me == 2, 2), (me == 4, 3), (me == 6, 4)):
            @pl.when(cond)
            def _(count=count):
                wait_for(h, recv_index(3, item), where(item, slice(0, count)))

    def arrivals_first():
        arrivals(None)
        if tree:
            @pl.when(odd)
            def _():
                wait_for(None, 2, dwin.at[:1])
                send_block().wait_recv()

    lane = lax.broadcasted_iota(jnp.int32, (shard_rows, shard_rows), 1)
    row = lax.broadcasted_iota(jnp.int32, (shard_rows, shard_rows), 0)
    doc_col = jnp.transpose(jnp.broadcast_to(dwin[own], (shard_rows, shard_rows)))

    def fill_bias(slot):
        off = reach - slot
        count = counts_ref[lax.max(me - off, 0)]
        docs = dwin[slot + 1]
        allowed = (docs == doc_col) & (lane < count)
        if off == 0:
            allowed = allowed & (lane <= row)
        part = jnp.where(allowed, 0.0, NEG).astype(jnp.float32)
        part = jnp.broadcast_to(part[:, None, :], (shard_rows, group, shard_rows))
        bias[:, slot * shard_rows : (slot + 1) * shard_rows] = part.reshape(rows, shard_rows)

    own_count = counts_ref[me]
    factor = math.log2(math.e) / math.sqrt(width)
    remote = reach * shard_rows

    def scores(h, start, keys):
        q = q_vmem[h, start // group : (start + tile) // group].reshape(tile, width)
        return lax.dot_general(
            q, keys, (((1,), (1,)), ((), ())), preferred_element_type=jnp.float32
        )

    def own_scores(h):
        q = q_vmem[h].reshape(rows, width)
        return lax.dot_general(
            q, win[h, 0, own], (((1,), (1,)), ((), ())), preferred_element_type=jnp.float32
        )

    def own_weights(h, s):
        x = s * factor + bias[:, remote:]
        top = jnp.max(x, axis=-1, keepdims=True)
        top_ref[h] = jnp.broadcast_to(top, (rows, width))
        return jnp.exp2(x - top)

    def own_mix(h, p):
        ones = jnp.ones((shard_rows, width), jnp.bfloat16)
        o = mix(p, jnp.concatenate([win[h, 1, own], ones], axis=1))
        part_ref[h] = o[:, :width]
        norm_ref[h] = o[:, width:]

    def attend_own(i):
        hs = [i * together + u for u in range(together)]
        s, p = {}, {}
        for k in range(together + 2):
            if k < together:
                s[k] = own_scores(hs[k])
            if 1 <= k <= together:
                p[k - 1] = own_weights(hs[k - 1], s.pop(k - 1))
            if k >= 2:
                own_mix(hs[k - 2], p.pop(k - 2))

    def attend_keys(h):
        keys = win[h, 0, 1:own].reshape(remote, width)
        s_next = scores(h, 0, keys)
        for start in range(0, rows, tile):
            at = slice(start, start + tile)
            s = s_next
            if start + tile < rows:
                s_next = scores(h, start + tile, keys)
            x = s * factor + bias[at, :remote]
            own_top = top_ref[h, at]
            top = jnp.maximum(jnp.max(x, axis=-1, keepdims=True), own_top)
            p = jnp.exp2(x - jnp.concatenate([top] * reach, axis=1))
            scale = jnp.exp2(own_top - top)
            weights[at] = p.astype(jnp.bfloat16)
            top_ref[h, at] = scale
            norm = jnp.sum(p, axis=-1, keepdims=True) + scale * norm_ref[h, at]
            r = lax.broadcasted_iota(jnp.int32, (tile, width), 0) + start
            norm_ref[h, at] = jnp.where(r < own_count * group, norm, jnp.inf)

    def attend_values(h):
        for start in range(0, rows, tile):
            at = slice(start, start + tile)
            out_ref[start // group : (start + tile) // group, h] = mixed(
                weights[at], win[h, 1, 1:own].reshape(remote, width),
                top_ref[h, at], part_ref[h, at], norm_ref[h, at],
            ).reshape(tile // group, group, width)

    shift = first_head(n, tree)

    def order(i):
        return lax.rem(i + shift, heads)

    fill_bias(reach)
    pltpu.make_async_copy(q_vmem, q_vmem, q_sem.at[0]).wait()
    loop(attend_own, heads // together)
    if tree:
        for item in (None, (order(0), 0), (order(0), 1)):
            fetch(item)
    arrivals_first()
    for slot in range(reach):
        fill_bias(slot)

    def step(i):
        h = order(i)
        for part in range(2):
            if tree:
                ready = (i + ahead > 0) & (i + ahead < heads)
                early = ready & (i == heads - 1)

                @pl.when(ready if part == 0 else ready & jnp.logical_not(early))
                def _(part=part):
                    fetch((order(i + ahead), part))

                if part == 0:
                    @pl.when(early)
                    def _():
                        fetch((h, 1))

            if tree:
                arrivals((h, part))
            elif part == 0:
                arrivals((h, both))
            if part == 0:
                attend_keys(h)
            else:
                @pl.when(i < heads - 1)
                def _():
                    attend_values(h)

    loop(step)
    last_values[...] = win[order(heads - 1), 1, 1:own].reshape(remote, width)

    one, two = win.at[:, :, own], win.at[:, :, :2]
    ends = [(kind, cond, one, 1) for kind, cond, _, _ in own_sends]
    if tree:
        ends += [
            (3, odd & (me >= 3), two, 2),
            (4, me == 5, one, 1),
            (4, last_odd, two, 2),
            (5, last_odd, win.at[1:, :, :2], 0),
            (6, straight, win.at[0, :, own], 1),
        ]
    for kind, cond, ref, _ in ends:
        @pl.when(cond)
        def _(kind=kind, ref=ref):
            wait_sent(send_sem.at[kind], ref)

    sent = sum(jnp.where(cond, docs, 0) for _, cond, _, docs in ends)
    for count in range(1, max(reach, 4) + 1):
        @pl.when(sent == count)
        def _(count=count):
            wait_sent(dsend_sem.at[0], dwin.at[:count])


def local(n, queries, keys, values, doc_ids, counts):
    shard_rows, q_heads, width = queries.shape
    heads = keys.shape[1]
    group = q_heads // heads
    reach = min((DOC_MOST + shard_rows - 1) // shard_rows, n - 1)
    rows = shard_rows * group
    tree = n == 8 and reach == 4
    shape = (shard_rows, heads, group, width)
    remote = reach * shard_rows
    saved = pltpu.VMEM((heads, rows, width), jnp.float32)
    outs = pl.pallas_call(
        functools.partial(kernel, n, reach, 512),
        out_shape=(
            pltpu.VMEM(shape, jnp.bfloat16),
            pltpu.VMEM((rows, remote), jnp.bfloat16),
            saved,
            saved,
            saved,
            pltpu.VMEM((remote, width), jnp.bfloat16),
        ),
        in_specs=[pl.BlockSpec(memory_space=pltpu.HBM)] * 5,
        out_specs=[pl.BlockSpec(memory_space=pltpu.VMEM)] * 6,
        scratch_shapes=[
            pltpu.VMEM((2, shard_rows, heads, width), jnp.bfloat16),
            pltpu.VMEM((heads, 2, reach + 2, shard_rows, width), jnp.bfloat16),
            pltpu.VMEM((heads, shard_rows, group, width), jnp.bfloat16),
            pltpu.VMEM((reach + 2, 1, shard_rows), jnp.int32),
            pltpu.VMEM((rows, (reach + 1) * shard_rows), jnp.float32),
            pltpu.SMEM(counts.shape, jnp.int32),
            pltpu.SemaphoreType.DMA((2,)),
            pltpu.SemaphoreType.DMA((1,)),
            pltpu.SemaphoreType.DMA((1,)),
            pltpu.SemaphoreType.DMA((7,)),
            pltpu.SemaphoreType.DMA((heads, max(reach, 4))),
            pltpu.SemaphoreType.DMA((1,)),
            pltpu.SemaphoreType.DMA((1,)),
            pltpu.SemaphoreType.DMA((max(reach, 3),)),
        ],
        compiler_params=pltpu.CompilerParams(
            collective_id=0, has_side_effects=True, vmem_limit_bytes=30 << 20
        ),
    )(
        *(
            pltpu.with_memory_space_constraint(x, pltpu.HBM)
            for x in (
                counts,
                queries.reshape(shard_rows, heads, group, width),
                keys,
                values,
                doc_ids.reshape(1, shard_rows),
            )
        )
    )
    out = pl.pallas_call(
        functools.partial(finish_kernel, n, tree, 512),
        out_shape=jax.ShapeDtypeStruct(shape, jnp.bfloat16),
        in_specs=[pl.BlockSpec(memory_space=pltpu.VMEM)] * 6,
        out_specs=pl.BlockSpec(memory_space=pltpu.HBM),
        scratch_shapes=[
            pltpu.VMEM((shard_rows, group, width), jnp.bfloat16),
            pltpu.SemaphoreType.DMA((2,)),
        ],
        compiler_params=pltpu.CompilerParams(vmem_limit_bytes=16 << 20),
    )(*(pltpu.with_memory_space_constraint(x, pltpu.VMEM) for x in outs))
    return out.reshape(shard_rows, q_heads, width)


def solution(mesh):
    in_specs = (
        P(("dp", "seq"), None, None),
        P(("dp", "seq"), None, None),
        P(("dp", "seq"), None, None),
        P(("dp", "seq")),
        P("dp"),
    )
    out_specs = P(("dp", "seq"), None, None)
    return jax.shard_map(
        functools.partial(local, mesh.shape["seq"]),
        mesh=mesh, in_specs=in_specs, out_specs=out_specs, check_vma=False,
    )
```

```python
import functools
import math

import jax
import jax.numpy as jnp
from jax import lax
from jax.experimental import pallas as pl
from jax.experimental.pallas import tpu as pltpu
from jax.sharding import PartitionSpec as P

DOC_MOST = 512
MESH = pl.DeviceIdType.MESH
NEG = -1e30


def mix(p, values):
    return lax.dot_general(
        p.astype(jnp.bfloat16), values, (((1,), (0,)), ((), ())),
        preferred_element_type=jnp.float32,
    )


def mixed(weights, values, scale, part, norm):
    return ((mix(weights, values) + scale * part) / norm).astype(jnp.bfloat16)


def first_head(n, tree):
    return jnp.where(lax.axis_index("seq") >= 6, 1, 0) if tree else 0


def finish_kernel(
    n, tree, tile,
    mixed_ref, weights, top_ref, norm_ref, part_ref, values, out_hbm, last, sem,
):
    rows, remote = weights.shape
    shard_rows, heads, group, width = mixed_ref.shape
    first = first_head(n, tree)

    def copy(i, c):
        h = lax.rem(i + first, heads)
        pltpu.make_async_copy(mixed_ref.at[:, h], out_hbm.at[:, h], sem.at[0]).start()
        return c

    lax.fori_loop(0, heads - 1, copy, 0)
    h = lax.rem(heads - 1 + first, heads)
    for start in range(0, rows, tile):
        at = slice(start, start + tile)
        places = slice(start // group, (start + tile) // group)
        last[places] = mixed(
            weights[at], values[...], top_ref[h, at], part_ref[h, at], norm_ref[h, at],
        ).reshape(tile // group, group, width)
        pltpu.make_async_copy(last.at[places], out_hbm.at[places, h], sem.at[1]).start()
    rest = mixed_ref.at[:, 1:]
    pltpu.make_async_copy(rest, rest, sem.at[0]).wait()
    pltpu.make_async_copy(last, last, sem.at[1]).wait()


def kernel(
    n, reach, tile,
    counts_hbm, q_hbm, k_hbm, v_hbm, docs_hbm,
    out_ref, weights, top_ref, norm_ref, part_ref, last_values,
    raw, win, q_vmem, dwin, bias, counts_ref, small_sem, raw_sem,
    q_sem, send_sem, recv_sem, block_sem, dsend_sem, drecv_sem,
):
    me = lax.axis_index("seq")
    heads, shard_rows, group, width = q_vmem.shape
    together = math.gcd(heads, 4)
    own = reach + 1
    rows = shard_rows * group
    tree = n == 8 and reach == 4

    even = lax.rem(me, 2) == 0
    odd = jnp.logical_not(even)
    chip_odd = lax.rem(me // 2, 2) == 1
    partner = me + 1 - 2 * lax.rem(me, 2)
    if tree:
        straight = (me == 2) | (me == 3)
        last_odd = me == 7
        send_shift = jnp.where(me >= 2, 1, 0)
        ahead = jnp.where(last_odd, 1, 0)
        own_sends = [
            (0, jnp.logical_not(chip_odd), jnp.where(even, me + 3, me + 2), jnp.where(even, 2, 3)),
            (1, me < 4, jnp.where(me < 2, me + 4, 7), jnp.where(me == 2, 0, 1)),
            (2, even, me + 1, reach),
        ]
        straight_slot = jnp.where(me == 2, 2, 3)
        senders = [
            (odd | (me >= 2), partner),
            (lax.rem(me, 4) == 3, me - 3),
            (lax.rem(me, 4) == 3, me - 2),
            ((me == 4) | (me == 5), me - 4),
            (last_odd, 2),
            (last_odd, 3),
            (me == 5, 7),
            (me == 5, 2),
            (me == 5, 3),
        ]
        targets = [
            even, odd & (me >= 3), jnp.logical_not(chip_odd), me < 4, last_odd, straight,
        ]
    else:
        own_sends = [
            (off - 1, me + off < n, lax.rem(me + off, n), own - off)
            for off in range(1, reach + 1)
        ]
        senders = [(me >= off, me - off) for off in range(1, reach + 1)]
        targets = [me + off < n for off in range(1, reach + 1)]
        send_shift = 0

    barrier = pltpu.get_barrier_semaphore()
    for cond, device in senders:
        @pl.when(cond)
        def _(device=device):
            pl.semaphore_signal(
                barrier, inc=1, device_id={"seq": lax.rem(device + n, n)},
                device_id_type=MESH,
            )

    def loop(body, count=None):
        lax.fori_loop(0, heads if count is None else count, lambda i, c: (body(i), c)[1], 0)

    raw_copies = [
        pltpu.make_async_copy(ref, raw.at[part], raw_sem.at[0])
        for part, ref in enumerate((k_hbm, v_hbm))
    ]
    doc_copy = pltpu.make_async_copy(docs_hbm, dwin.at[own], small_sem.at[0])
    count_copy = pltpu.make_async_copy(counts_hbm, counts_ref, small_sem.at[1])
    doc_copy.start()
    for copy in raw_copies:
        copy.start()
    count_copy.start()

    def q_copy(h):
        return pltpu.make_async_copy(q_hbm.at[:, h], q_vmem.at[h], q_sem.at[0])

    loop(lambda h: q_copy(h).start())

    both = slice(0, 2)

    def where(item, slot):
        if item is None:
            return dwin.at[slot]
        return win.at[item[0], item[1], slot]

    def recv_index(kind, item):
        if not tree:
            return kind
        if item is None:
            return {1: 1, 2: 2}.get(kind, 0)
        return (2 if kind == 1 else 0) + item[1]

    def send(item, kind, slot, to, to_slot):
        index = recv_index(kind, item)
        return pltpu.make_async_remote_copy(
            src_ref=where(item, slot), dst_ref=where(item, to_slot),
            send_sem=dsend_sem.at[0] if item is None else send_sem.at[0],
            recv_sem=drecv_sem.at[index] if item is None else recv_sem.at[item[0], index],
            device_id={"seq": to}, device_id_type=MESH,
        )

    def send_block():
        return pltpu.make_async_remote_copy(
            src_ref=win.at[:, :, own], dst_ref=win.at[:, :, reach],
            send_sem=send_sem.at[0], recv_sem=block_sem.at[0],
            device_id={"seq": partner}, device_id_type=MESH,
        )

    def wait_for(h, index, ref):
        pltpu.make_async_remote_copy(
            src_ref=ref, dst_ref=ref, send_sem=send_sem.at[0],
            recv_sem=drecv_sem.at[index] if h is None else recv_sem.at[h, index],
            device_id={"seq": lax.rem(me + 1, n)}, device_id_type=MESH,
        ).wait_recv()

    def wait_sent(sem, ref):
        pltpu.make_async_remote_copy(
            src_ref=ref, dst_ref=ref, send_sem=sem, recv_sem=recv_sem.at[0, 0],
            device_id={"seq": lax.rem(me + 1, n)}, device_id_type=MESH,
        ).wait_send()

    def start_own(h):
        for kind, cond, to, slot in own_sends:
            if h is not None and tree and kind == 2:
                continue
            parts = [0, 1] if tree else [both]
            for item in [None] if h is None else [(h, part) for part in parts]:
                @pl.when(cond)
                def _(item=item, kind=kind, to=to, slot=slot):
                    send(item, kind, own, to, slot).start()

    doc_copy.wait()
    pltpu.make_async_copy(raw, raw, raw_sem.at[0]).wait()
    for part in range(2):
        win[:, part, own] = jnp.swapaxes(raw[part], 0, 1)
    pl.semaphore_wait(barrier, sum(jnp.where(cond, 1, 0) for cond in targets))

    start_own(None)
    if tree:
        @pl.when(straight)
        def _():
            for item in (None, (0, 0), (0, 1)):
                send(item, 6, own, 5, straight_slot).start()

    def start_head(i):
        start_own(lax.rem(i + send_shift, heads))

    loop(start_head)
    if tree:
        @pl.when(even)
        def _():
            send_block().start()

    count_copy.wait()

    for off in range(1, reach + 1):
        @pl.when(me < off)
        def _(off=off):
            dwin[own - off] = jnp.full(dwin.shape[1:], -1, jnp.int32)

            def clear(h):
                win[h, :, own - off] = jnp.zeros((2, shard_rows, width), win.dtype)

            loop(clear)

    def fetch_y(item):
        h = None if item is None else item[0]
        index = recv_index(1, item)
        two = slice(0, 2)

        @pl.when(last_odd)
        def _():
            wait_for(h, index, where(item, two))
            if item is not None:
                @pl.when(h > 0)
                def _():
                    send(item, 5, two, 5, slice(2, 4)).start()

            send(item, 4, two, 6, slice(1, 3)).start()

        @pl.when(me == 5)
        def _():
            wait_for(h, index, where(item, 1))
            send(item, 4, 1, 4, 2).start()

    def fetch(item):
        fetch_y(item)

        @pl.when(odd & (me >= 3))
        def _():
            h = None if item is None else item[0]
            wait_for(h, recv_index(0, item), where(item, slice(0, 2)))
            send(item, 3, slice(2, 4), me - 1, slice(3, 5)).start()

    def arrivals(item):
        h = None if item is None else item[0]
        if not tree:
            for off in range(1, reach + 1):
                @pl.when(me >= off)
                def _(off=off):
                    wait_for(h, off - 1, where(item, slice(0, 1)))
            return

        @pl.when(me == 4)
        def _():
            wait_for(h, recv_index(1, item), where(item, 1))

        for cond, count in ((me == 2, 2), (me == 4, 3), (me == 6, 4)):
            @pl.when(cond)
            def _(count=count):
                wait_for(h, recv_index(3, item), where(item, slice(0, count)))

    def arrivals_first():
        arrivals(None)
        if tree:
            @pl.when(odd)
            def _():
                wait_for(None, 2, dwin.at[:1])
                send_block().wait_recv()

    lane = lax.broadcasted_iota(jnp.int32, (shard_rows, shard_rows), 1)
    row = lax.broadcasted_iota(jnp.int32, (shard_rows, shard_rows), 0)
    doc_col = jnp.transpose(jnp.broadcast_to(dwin[own], (shard_rows, shard_rows)))

    def fill_bias(slot):
        off = reach - slot
        count = counts_ref[lax.max(me - off, 0)]
        docs = dwin[slot + 1]
        allowed = (docs == doc_col) & (lane < count)
        if off == 0:
            allowed = allowed & (lane <= row)
        part = jnp.where(allowed, 0.0, NEG).astype(jnp.float32)
        part = jnp.broadcast_to(part[:, None, :], (shard_rows, group, shard_rows))
        bias[:, slot * shard_rows : (slot + 1) * shard_rows] = part.reshape(rows, shard_rows)

    own_count = counts_ref[me]
    factor = math.log2(math.e) / math.sqrt(width)
    remote = reach * shard_rows

    def scores(h, start, keys):
        q = q_vmem[h, start // group : (start + tile) // group].reshape(tile, width)
        return lax.dot_general(
            q, keys, (((1,), (1,)), ((), ())), preferred_element_type=jnp.float32
        )

    def own_scores(h):
        q = q_vmem[h].reshape(rows, width)
        return lax.dot_general(
            q, win[h, 0, own], (((1,), (1,)), ((), ())), preferred_element_type=jnp.float32
        )

    def own_weights(h, s):
        x = s * factor + bias[:, remote:]
        top = jnp.max(x, axis=-1, keepdims=True)
        top_ref[h] = jnp.broadcast_to(top, (rows, width))
        return jnp.exp2(x - top)

    def own_mix(h, p):
        ones = jnp.ones((shard_rows, width), jnp.bfloat16)
        o = mix(p, jnp.concatenate([win[h, 1, own], ones], axis=1))
        part_ref[h] = o[:, :width]
        norm_ref[h] = o[:, width:]

    def attend_own(i):
        hs = [i * together + u for u in range(together)]
        s, p = {}, {}
        for k in range(together + 2):
            if k < together:
                s[k] = own_scores(hs[k])
            if 1 <= k <= together:
                p[k - 1] = own_weights(hs[k - 1], s.pop(k - 1))
            if k >= 2:
                own_mix(hs[k - 2], p.pop(k - 2))

    def attend_keys(h):
        keys = win[h, 0, 1:own].reshape(remote, width)
        s_next = scores(h, 0, keys)
        for start in range(0, rows, tile):
            at = slice(start, start + tile)
            s = s_next
            if start + tile < rows:
                s_next = scores(h, start + tile, keys)
            x = s * factor + bias[at, :remote]
            own_top = top_ref[h, at]
            top = jnp.maximum(jnp.max(x, axis=-1, keepdims=True), own_top)
            p = jnp.exp2(x - jnp.concatenate([top] * reach, axis=1))
            scale = jnp.exp2(own_top - top)
            weights[at] = p.astype(jnp.bfloat16)
            top_ref[h, at] = scale
            norm = jnp.sum(p, axis=-1, keepdims=True) + scale * norm_ref[h, at]
            r = lax.broadcasted_iota(jnp.int32, (tile, width), 0) + start
            norm_ref[h, at] = jnp.where(r < own_count * group, norm, jnp.inf)

    def attend_values(h):
        for start in range(0, rows, tile):
            at = slice(start, start + tile)
            out_ref[start // group : (start + tile) // group, h] = mixed(
                weights[at], win[h, 1, 1:own].reshape(remote, width),
                top_ref[h, at], part_ref[h, at], norm_ref[h, at],
            ).reshape(tile // group, group, width)

    shift = first_head(n, tree)

    def order(i):
        return lax.rem(i + shift, heads)

    fill_bias(reach)
    pltpu.make_async_copy(q_vmem, q_vmem, q_sem.at[0]).wait()
    loop(attend_own, heads // together)
    if tree:
        for item in (None, (order(0), 0), (order(0), 1)):
            fetch(item)
    arrivals_first()
    for slot in range(reach):
        fill_bias(slot)

    def step(i):
        h = order(i)
        for part in range(2):
            if tree:
                ready = (i + ahead > 0) & (i + ahead < heads)
                early = ready & (i == heads - 1)

                @pl.when(ready if part == 0 else ready & jnp.logical_not(early))
                def _(part=part):
                    fetch((order(i + ahead), part))

                if part == 0:
                    @pl.when(early)
                    def _():
                        fetch((h, 1))

            if tree:
                arrivals((h, part))
            elif part == 0:
                arrivals((h, both))
            if part == 0:
                attend_keys(h)
            else:
                @pl.when(i < heads - 1)
                def _():
                    attend_values(h)

    loop(step)
    last_values[...] = win[order(heads - 1), 1, 1:own].reshape(remote, width)

    one, two = 2 * heads, 4 * heads
    ends = [(cond, one, 1) for _, cond, _, _ in own_sends]
    totals = {one * count for count in range(1, reach + 1)}
    if tree:
        ends += [
            (odd & (me >= 3), two, 2),
            (me == 5, one, 1),
            (last_odd, two, 2),
            (last_odd, two - 4, 0),
            (straight, 2, 1),
        ]
        totals |= {2 * one + 2, two + one + 2, 3 * two - 4}
    total = sum(jnp.where(cond, blocks, 0) for cond, blocks, _ in ends)
    for count in sorted(totals):
        @pl.when(total == count)
        def _(count=count):
            wait_sent(send_sem.at[0], part_ref.at[:, : count * shard_rows // (2 * heads)])

    sent = sum(jnp.where(cond, docs, 0) for cond, _, docs in ends)
    for count in range(1, max(reach, 4) + 1):
        @pl.when(sent == count)
        def _(count=count):
            wait_sent(dsend_sem.at[0], dwin.at[:count])


def local(n, queries, keys, values, doc_ids, counts):
    shard_rows, q_heads, width = queries.shape
    heads = keys.shape[1]
    group = q_heads // heads
    reach = min((DOC_MOST + shard_rows - 1) // shard_rows, n - 1)
    rows = shard_rows * group
    tree = n == 8 and reach == 4
    shape = (shard_rows, heads, group, width)
    remote = reach * shard_rows
    saved = pltpu.VMEM((heads, rows, width), jnp.float32)
    outs = pl.pallas_call(
        functools.partial(kernel, n, reach, 512),
        out_shape=(
            pltpu.VMEM(shape, jnp.bfloat16),
            pltpu.VMEM((rows, remote), jnp.bfloat16),
            saved,
            saved,
            saved,
            pltpu.VMEM((remote, width), jnp.bfloat16),
        ),
        in_specs=[pl.BlockSpec(memory_space=pltpu.HBM)] * 5,
        out_specs=[pl.BlockSpec(memory_space=pltpu.VMEM)] * 6,
        scratch_shapes=[
            pltpu.VMEM((2, shard_rows, heads, width), jnp.bfloat16),
            pltpu.VMEM((heads, 2, reach + 2, shard_rows, width), jnp.bfloat16),
            pltpu.VMEM((heads, shard_rows, group, width), jnp.bfloat16),
            pltpu.VMEM((reach + 2, 1, shard_rows), jnp.int32),
            pltpu.VMEM((rows, (reach + 1) * shard_rows), jnp.float32),
            pltpu.SMEM(counts.shape, jnp.int32),
            pltpu.SemaphoreType.DMA((2,)),
            pltpu.SemaphoreType.DMA((1,)),
            pltpu.SemaphoreType.DMA((1,)),
            pltpu.SemaphoreType.DMA((1,)),
            pltpu.SemaphoreType.DMA((heads, max(reach, 4))),
            pltpu.SemaphoreType.DMA((1,)),
            pltpu.SemaphoreType.DMA((1,)),
            pltpu.SemaphoreType.DMA((max(reach, 3),)),
        ],
        compiler_params=pltpu.CompilerParams(
            collective_id=0, has_side_effects=True, vmem_limit_bytes=30 << 20
        ),
    )(
        *(
            pltpu.with_memory_space_constraint(x, pltpu.HBM)
            for x in (
                counts,
                queries.reshape(shard_rows, heads, group, width),
                keys,
                values,
                doc_ids.reshape(1, shard_rows),
            )
        )
    )
    out = pl.pallas_call(
        functools.partial(finish_kernel, n, tree, 512),
        out_shape=jax.ShapeDtypeStruct(shape, jnp.bfloat16),
        in_specs=[pl.BlockSpec(memory_space=pltpu.VMEM)] * 6,
        out_specs=pl.BlockSpec(memory_space=pltpu.HBM),
        scratch_shapes=[
            pltpu.VMEM((shard_rows, group, width), jnp.bfloat16),
            pltpu.SemaphoreType.DMA((2,)),
        ],
        compiler_params=pltpu.CompilerParams(vmem_limit_bytes=16 << 20),
    )(*(pltpu.with_memory_space_constraint(x, pltpu.VMEM) for x in outs))
    return out.reshape(shard_rows, q_heads, width)


def solution(mesh):
    in_specs = (
        P(("dp", "seq"), None, None),
        P(("dp", "seq"), None, None),
        P(("dp", "seq"), None, None),
        P(("dp", "seq")),
        P("dp"),
    )
    out_specs = P(("dp", "seq"), None, None)
    return jax.shard_map(
        functools.partial(local, mesh.shape["seq"]),
        mesh=mesh, in_specs=in_specs, out_specs=out_specs, check_vma=False,
    )
```
